32 devices in a mesh: row: 16 (over z, x, core), col: 2 (over y).
Axes of the slice: x: 2, y: 2, z: 4, core: 2. Of those that a mesh axis runs over, the one named last changes fastest.
Arguments:
- occupied_waves: bfloat16 [1024, 32768], P('row', 'col'), may hold values from -6 to 6
- virtual_waves: bfloat16 [512, 32768], P('row', 'col'), may hold values from -6 to 6
- occupied_decay: float32 [1024], replicated, may hold values from 0.02 to 1
- virtual_decay: float32 [512], replicated, may hold values from 0.02 to 1
Outputs:
- spectrum_real: float32 [512, 32, 1024], P('row', 'col')
- spectrum_imaginary: float32 [512, 32, 1024], P('row', 'col')
The draws below stay inside these ranges and needn't reach their ends.
All inputs are finite; a program needn't handle non-finite values.
Results may differ from the reference program's by a relative error of at most 0.0041.
Values may be sent and summed in bfloat16 or wider, within the bound.
A program may use at most 128 MiB of HBM per device.

```python
import math
import jax
import jax.numpy as jnp
from jax import lax

NOCC = 1024
NVIR = 512
NA = 32
NB = 32
NC = 32
ROWS_DEV = 32
NGRID = 32768
N_ROW = 16


def steps_of(key, dims, pieces, smallest, high):
    loudness, own = 1.0, jax.random.fold_in(key, 6)
    for position, parts in pieces:
        heights = jnp.exp(jax.random.uniform(jax.random.fold_in(own, position), (parts,), jnp.float32, smallest / len(pieces), high / len(pieces)))
        loudness = loudness * jnp.repeat(heights, dims[position] // parts).reshape([-1 if axis == position else 1 for axis in range(len(dims))])
    return loudness


def noise(rng, extent, scale, limit, split=(), kind=jnp.bfloat16):
    drawn = scale * jax.random.normal(rng, extent, jnp.float32)
    if split:
        drawn = drawn * steps_of(rng, extent, split, -0.22, 0.18)
    return jnp.clip(drawn, -limit, limit).astype(kind)


def setup_inputs(seed: int = 0) -> dict:
    keys = jax.random.split(jax.random.key(seed), 5)
    return {
        "occupied_waves": noise(keys[0], (NOCC, NGRID), 1.0, 6.0, ((0, 16), (1, 2))),
        "virtual_waves": noise(keys[1], (NVIR, NGRID), 1.0, 6.0, ((0, 16), (1, 2))),
        "occupied_decay": jnp.clip(jnp.exp(jax.random.uniform(keys[2], (NOCC,), jnp.float32, math.log(0.02), math.log(1.0))), 0.02, 1.0),
        "virtual_decay": jnp.clip(jnp.exp(jax.random.uniform(keys[3], (NVIR,), jnp.float32, math.log(0.02), math.log(1.0))), 0.02, 1.0),
    }


def reference(occupied_waves, virtual_waves, occupied_decay, virtual_decay):
    rows_all = ROWS_DEV * N_ROW
    width = math.gcd(rows_all, 512)
    factor = -1.0 / math.sqrt(NOCC * NVIR)
    contract = (((0,), (0,)), ((), ()))

    def block(index):
        first = (index * width).astype(jnp.int32)
        occ_rows = lax.dynamic_slice_in_dim(occupied_waves, first, width, 1)
        occ_rows = (occ_rows.astype(jnp.float32) * occupied_decay[:, None]).astype(jnp.bfloat16)
        vir_rows = lax.dynamic_slice_in_dim(virtual_waves, first, width, 1)
        vir_rows = (vir_rows.astype(jnp.float32) * virtual_decay[:, None]).astype(jnp.bfloat16)
        green_occ = lax.dot_general(occupied_waves, occ_rows, contract, preferred_element_type=jnp.float32)
        green_vir = lax.dot_general(virtual_waves, vir_rows, contract, preferred_element_type=jnp.float32)
        polar = green_occ * green_vir * factor
        cube = polar.reshape(NA, NB, NC, width)
        spectrum = jnp.fft.fftn(cube, axes=(0, 1, 2)) / math.sqrt(NGRID)
        spectrum = jnp.transpose(spectrum, (3, 2, 0, 1)).reshape(width, NC, NA * NB)
        return (jnp.real(spectrum).astype(jnp.float32), jnp.imag(spectrum).astype(jnp.float32))
    real_part, imag_part = lax.map(block, jnp.arange(rows_all // width, dtype=jnp.int32))
    real_part = real_part.reshape(rows_all, NC, NA * NB)
    imag_part = imag_part.reshape(rows_all, NC, NA * NB)
    return (real_part, imag_part)
```

```python
import functools
import math

import jax
import jax.numpy as jnp
import numpy as np
from jax import lax
from jax.experimental import pallas as pl
from jax.experimental.pallas import tpu as pltpu
from jax.sharding import PartitionSpec as P

NA = 32
NB = 32
NC = 32
NAB = NA * NB
NGRID = NA * NB * NC
LANES = 128
R_BLOCK = 16


def trig(phase, length):
    angle = (phase % length) * (2.0 * math.pi / length)
    return np.cos(angle), np.sin(angle)


def bf16_table(table):
    return jnp.asarray(table.astype(np.float32)).astype(jnp.bfloat16)


def plane_tables():
    index = np.arange(NAB)
    a, b = index // NB, index % NB
    phase = a[:, None] * a[None, :] * NB + b[:, None] * b[None, :] * NA
    cosine, sine = trig(phase, NA * NB)
    return bf16_table(cosine), bf16_table(sine)


def line_tables(col_count):
    share = NC // col_count
    full = np.zeros((col_count, 2, R_BLOCK, share, NC, R_BLOCK))
    for y in range(col_count):
        kc = y * share + np.arange(share)
        cosine, sine = trig(kc[:, None] * np.arange(NC)[None, :], NC)
        for r in range(R_BLOCK):
            full[y, 0, r, :, :, r] = cosine
            full[y, 1, r, :, :, r] = -sine
    return bf16_table(full.reshape(col_count, 2 * R_BLOCK * share, NC * R_BLOCK))


def dot(a, b):
    return jnp.dot(a, b, preferred_element_type=jnp.float32)


def spectrum_kernel(x_ref, line_ref, cos_ref, sin_ref, re_ref, im_ref):
    rows = x_ref[...].reshape(NC * R_BLOCK, NAB)
    line = dot(line_ref[lax.axis_index("col")], rows).astype(jnp.bfloat16)
    half = line.shape[0] // 2
    re, im = line[:half], line[half:]
    re_ref[...] = dot(re, cos_ref[...]) + dot(im, sin_ref[...])
    im_ref[...] = dot(im, cos_ref[...]) - dot(re, sin_ref[...])


def spectrum(x, line_table):
    r_count = x.shape[1]
    cosine, sine = plane_tables()
    out_rows = line_table.shape[1] // 2
    steps = r_count // R_BLOCK
    whole = lambda table: pl.BlockSpec(table.shape, lambda i: (0,) * table.ndim)
    out = jax.ShapeDtypeStruct((out_rows * steps, NAB), jnp.float32)
    out_spec = pl.BlockSpec((out_rows, NAB), lambda i: (i, 0))
    return pl.pallas_call(
        spectrum_kernel,
        grid=(steps,),
        in_specs=[
            pl.BlockSpec((x.shape[0], R_BLOCK, x.shape[2]), lambda i: (0, i, 0)),
            whole(line_table),
            whole(cosine),
            whole(sine),
        ],
        out_specs=[out_spec, out_spec],
        out_shape=[out, out],
        compiler_params=pltpu.CompilerParams(vmem_limit_bytes=48 * 1024 * 1024),
    )(x, line_table, cosine, sine)


MESH = pl.DeviceIdType.MESH
HALVES = 2
HALF_ROWS = R_BLOCK


def flip(index, mask):
    bits = [1 << bit for bit in range(mask.bit_length()) if mask >> bit & 1]
    for bit in bits:
        index = index + bit - 2 * bit * lax.rem(lax.div(index, bit), 2)
    return index


def group_size(row_count):
    return 4 if row_count % 4 == 0 else 1


def send(src, dst, send_sem, recv_sem, target):
    return pltpu.make_async_remote_copy(
        src_ref=src,
        dst_ref=dst,
        send_sem=send_sem,
        recv_sem=recv_sem,
        device_id=target,
        device_id_type=MESH,
    )


def enter(row_count, col_count, inner, row, col):
    barrier = pltpu.get_barrier_semaphore()
    mine, seat = lax.div(row, inner), lax.rem(row, inner)
    targets = [(lax.rem(row + k, row_count), col) for k in range(1, row_count)]
    targets += [
        (mine * inner + lax.rem(seat + s, inner), lax.rem(col + d, col_count))
        for d in range(1, col_count)
        for s in range(inner)
    ]
    for target in targets:
        pl.semaphore_signal(barrier, inc=1, device_id=target, device_id_type=MESH)
    return barrier, len(targets)


def fill(ref, values, rows):
    width = ref.shape[1]

    def step(i, carry):
        start = pl.multiple_of(i * rows, rows)
        row = lax.broadcasted_iota(jnp.int32, (rows, width), 0) + start
        lane = lax.broadcasted_iota(jnp.int32, (rows, width), 1)
        ref[pl.ds(start, rows), :] = jnp.where(values(row, lane), 1.0, 0.0).astype(jnp.bfloat16)
        return carry

    lax.fori_loop(0, ref.shape[0] // rows, step, 0)


def whole_kernel(cfg, *refs):
    (row_count, col_count, inner, cuts, factor, fused) = cfg
    refs = list(refs)
    take = lambda n: [refs.pop(0) for _ in range(n)]
    occ_ref, vir_ref, occ_decay, vir_decay = take(4)
    if fused:
        line_hbm, cos_hbm, sin_hbm = take(3)
        acc_re, acc_im = take(2)
    else:
        (x_ref,) = take(1)
    planes = take(2)
    raws = take(2)
    lefts = take(2)
    mixed, polar, swap = take(3)
    if fused:
        x_ref, piece_swap, line_ref, cos_ref, sin_ref, lines_buf = take(6)
        table_sem = take(1)[0]
    (wave_send, wave_recv, col_send, col_recv, line_send, line_recv, group_send, group_recv) = take(8)
    (give_send, give_recv, pass_send, pass_recv, local) = take(5)

    row, col = lax.axis_index("row"), lax.axis_index("col")
    outer = row_count // inner
    mine, seat = lax.div(row, inner), lax.rem(row, inner)
    points = occ_ref.shape[1] // row_count
    waves = (occ_ref, vir_ref)
    window = raws[0].shape[3]
    share = window // col_count
    block_rows = row_count * HALF_ROWS

    def peer(k):
        return flip(mine, k // inner) * inner + lax.rem(seat + k % inner, inner)

    def source(k):
        return flip(mine, k // inner) * inner + lax.rem(seat + inner - k % inner, inner)

    barrier, arrivals = enter(row_count, col_count, inner, row, col)

    own = []
    for i in range(2):
        lanes = pl.ds(pl.multiple_of(row * points, LANES), points)
        own.append(pltpu.make_async_copy(waves[i].at[:, lanes], planes[i].at[row], local.at[i]))
    if fused:
        own.append(pltpu.make_async_copy(line_hbm.at[col], line_ref, table_sem.at[0]))
        own.append(pltpu.make_async_copy(cos_hbm, cos_ref, table_sem.at[1]))
        own.append(pltpu.make_async_copy(sin_hbm, sin_ref, table_sem.at[2]))
    for copy in own:
        copy.start()
    pl.semaphore_wait(barrier, arrivals)

    waiting = []

    def start_waves(part):
        first, last = cuts[part], cuts[part + 1]
        for k in range(row_count - 1, 0, -1):
            to = peer(k)
            lanes = pl.ds(pl.multiple_of(to * points + first, LANES), last - first)
            for i in range(2):
                copy = send(
                    waves[i].at[:, lanes],
                    planes[i].at[row, :, pl.ds(first, last - first)],
                    wave_send.at[i, part, k],
                    wave_recv.at[i, part, k],
                    (to, col),
                )
                copy.start()
                waiting.append((part, copy))

    def wait_waves(part):
        for number, copy in waiting:
            if number == part:
                copy.wait_recv()

    parts = len(cuts) - 1

    def slab_share(c):
        return pl.ds(c * share, share) if isinstance(c, int) else pl.ds(pl.multiple_of(c * share, LANES), share)

    def over_col(i, c):
        return send(
            waves[i].at[:, slab_share(c)],
            raws[i].at[mine, seat, :, slab_share(c)],
            col_send.at[i, c],
            col_recv.at[i, 0],
            (row, c),
        )

    @pl.when(col == 0)
    def _():
        for i in range(2):
            for c in range(1, col_count):
                over_col(i, c).start()
            pltpu.make_async_copy(
                waves[i].at[:, slab_share(0)], raws[i].at[mine, seat, :, slab_share(0)], local.at[2 + i]
            ).start()

    start_waves(0)

    @pl.when(col == 0)
    def _():
        for i in range(2):
            pltpu.make_async_copy(
                waves[i].at[:, slab_share(0)], raws[i].at[mine, seat, :, slab_share(0)], local.at[2 + i]
            ).wait()

    if col_count > 1:

        @pl.when(col != 0)
        def _():
            for i in range(2):
                over_col(i, 1).wait_recv()

    sent = []
    held = [0]
    bits = [1 << bit for bit in reversed(range((outer - 1).bit_length()))]
    next_part = 1
    for bit in bits:
        to = (flip(mine, bit) * inner + seat, col)
        started = []
        for mask in held:
            for i in range(2):
                place = raws[i].at[flip(mine, mask), seat, :, slab_share(col)]
                k = bit + mask
                started.append(send(place, place, line_send.at[i, k], line_recv.at[i, k], to))
        for copy in started:
            copy.start()
        sent.extend(started)
        held = held + [mask + bit for mask in held]
        if next_part < parts - 1:
            start_waves(next_part)
            next_part += 1
        for copy in started:
            copy.wait_recv()
    groups = []
    for s in range(inner):
        for d in range(col_count):
            if s == 0 and d == 0:
                continue
            to = (mine * inner + lax.rem(seat + s, inner), lax.rem(col + d, col_count))
            for i in range(2):
                place = raws[i].at[:, seat, :, slab_share(col)]
                copy = send(place, place, group_send.at[i, s, d], group_recv.at[i, s, d], to)
                copy.start()
                groups.append(copy)
    while next_part < parts:
        start_waves(next_part)
        next_part += 1

    per_point = points // NC
    fill(swap, lambda p, n: n == (p & (NC - 1)) * per_point + lax.div(p, NC), min(LANES, points))
    if fused:
        per = LANES // NB
        inside = per * NB

        def piece(p, n):
            k, j, w = lax.div(p, inside), lax.div(p & (inside - 1), NB), p & (NB - 1)
            return n == j * inside + k * NB + w

        fill(piece_swap, piece, LANES)
        acc_re[...] = jnp.zeros_like(acc_re)
        acc_im[...] = jnp.zeros_like(acc_im)

    for copy in groups:
        copy.wait_recv()

    for i, decay in enumerate((occ_decay, vir_decay)):
        raw, left = raws[i], lefts[i]
        bands = raw.shape[2]
        join = max(1, LANES // (inner * bands))
        width = join * inner * bands

        def scale(m, carry, raw=raw, left=left, decay=decay, width=width, join=join):
            lanes = pl.ds(pl.multiple_of(m * width, width), width)
            factors = decay[:, lanes]
            for t in range(window // LANES):
                piece = raw[pl.ds(m * join, join), :, :, pl.ds(t * LANES, LANES)]
                turned = piece.reshape(width, LANES).astype(jnp.float32).T * factors
                turned = turned.astype(jnp.bfloat16)
                for s in range(LANES // HALF_ROWS):
                    q = (t * LANES + s * HALF_ROWS) // (HALVES * HALF_ROWS)
                    at = ((s % HALVES) * row_count + q) * HALF_ROWS
                    left[pl.ds(at, HALF_ROWS), lanes] = turned[s * HALF_ROWS : (s + 1) * HALF_ROWS]
            return carry

        lax.fori_loop(0, outer // join, scale, 0)

    def product(h, first, width):
        rows = pl.ds(h * block_rows, block_rows)
        lanes = pl.ds(first, width)
        green = []
        for i in range(2):
            wave = planes[i][:, :, lanes]
            wave = wave.reshape(wave.shape[0] * wave.shape[1], width)
            green.append(dot(lefts[i][rows, :], wave))
        value = (green[0] * green[1] * factor).astype(jnp.bfloat16)
        return dot(value, swap[lanes, :])

    for copy in own[:2]:
        copy.wait()
    for part in range(parts):
        wait_waves(part)
        first, width = cuts[part], cuts[part + 1] - cuts[part]
        for h in range(HALVES):
            moved = product(h, first, width)
            if part:
                moved = mixed[h] + moved
            if part < parts - 1:
                mixed[h] = moved
            else:
                polar[h] = moved.astype(jnp.bfloat16).reshape(row_count, HALF_ROWS, points)
                gives = []
                for k in range(row_count - 1, 0, -1):
                    to = peer(k)
                    copy = send(
                        polar.at[h, to],
                        x_ref.at[h, col, row],
                        give_send.at[h, k],
                        give_recv.at[h, k],
                        (to, col),
                    )
                    copy.start()
                    gives.append(copy)
                if h == 0:
                    early = gives
                else:
                    late = gives
    gives = [list(reversed(early)), list(reversed(late))]

    passes = [[], []]

    def hand_on(h, k, src, slot):
        for d in range(1, col_count):
            to = (row, lax.rem(col + d, col_count))
            copy = send(src, slot, pass_send.at[h, d, k], pass_recv.at[h, d, k], to)
            copy.start()
            passes[h].append((k, copy))

    def forward(h, k):
        gives[h][k - 1].wait_recv()
        slot = x_ref.at[h, col, source(k)]
        hand_on(h, k, slot, slot)

    keep = []
    for h in range(HALVES):
        here = x_ref.at[h, col, row]
        copy = pltpu.make_async_copy(polar.at[h, row], here, local.at[2 + h])
        copy.start()
        keep.append(copy)
        hand_on(h, 0, polar.at[h, row], here)
    near = row_count // 2
    for h in range(HALVES):
        for k in range(1, near):
            forward(h, k)
    for copy in keep:
        copy.wait()

    def wait_pass(h, ks):
        for k, copy in passes[h]:
            if k in ks:
                copy.wait_recv()

    if fused:
        for copy in own[2:]:
            copy.wait()
        per = LANES // NB
        side = lax.div(row, near)
        other = 1 - side

        def transform(h, c, z):
            wide = near * NB
            for g in range(near // per):
                parts = []
                for t in range(NC // per):
                    lanes = pl.ds(t * LANES, LANES)
                    parts.append(
                        jnp.concatenate(
                            [x_ref[h, c, z * near + g * per + k, :, lanes] for k in range(per)], axis=1
                        )
                    )
                moved = dot(jnp.concatenate(parts, axis=0), piece_swap[...]).astype(jnp.bfloat16)
                for t in range(NC // per):
                    for j in range(per):
                        lines_buf[
                            pl.ds((t * per + j) * R_BLOCK, R_BLOCK), pl.ds(g * LANES, LANES)
                        ] = moved[t * R_BLOCK : (t + 1) * R_BLOCK, j * LANES : (j + 1) * LANES]
            line = dot(line_ref[...], lines_buf[...]).astype(jnp.bfloat16)
            half = line.shape[0] // 2
            re, im = line[:half], line[half:]
            depth = pl.ds(pl.multiple_of((c * 2 + z) * wide, wide), wide)
            rows = pl.ds(pl.multiple_of(h * half, half), half)
            cosine, sine = cos_ref[depth, :], sin_ref[depth, :]
            acc_re[rows, :] += dot(re, cosine) + dot(im, sine)
            acc_im[rows, :] += dot(im, cosine) - dot(re, sine)

        def over(jobs):
            def step(i, carry):
                h, c, z = jobs(i)
                transform(h, c, z)
                return carry

            return step

        lax.fori_loop(0, HALVES, over(lambda i: (i, col, side)), 0)
    for k in range(near, row_count):
        forward(0, k)
    for h in range(HALVES):
        wait_pass(h, range(near))
    wait_pass(0, range(near, row_count))
    if fused:
        for d in range(1, col_count):
            there = lax.rem(col + d, col_count)
            lax.fori_loop(0, HALVES, over(lambda i, there=there: (i, there, side)), 0)
        for d in range(col_count):
            transform(0, lax.rem(col + d, col_count), other)
    for k in range(near, row_count):
        forward(1, k)
    if fused:
        transform(1, col, other)
    wait_pass(1, range(near, row_count))
    if fused:
        for d in range(1, col_count):
            transform(1, lax.rem(col + d, col_count), other)

    for _, copy in waiting:
        copy.wait_send()
    for copy in sent + groups + gives[0] + gives[1]:
        copy.wait_send()
    for h in range(HALVES):
        for _, copy in passes[h]:
            copy.wait_send()

    @pl.when(col == 0)
    def _():
        for i in range(2):
            for c in range(1, col_count):
                over_col(i, c).wait_send()

    if not fused:
        for copy in own[2:]:
            copy.wait()


def whole(row_count, col_count, occ, vir, occ_decay, vir_decay, window, factor):
    inner = group_size(row_count)
    outer = row_count // inner
    points = occ.shape[1] // row_count
    fused = points == NB * NC and row_count * col_count == NA and (row_count // 2) % (LANES // NB) == 0
    quarter = points // 4
    cuts = tuple(range(0, points + 1, quarter)) if quarter % LANES == 0 else (0, points)
    parts = len(cuts) - 1
    bands = (occ.shape[0], vir.shape[0])
    block_rows = row_count * HALF_ROWS
    bf16, f32 = jnp.bfloat16, jnp.float32
    dma = pltpu.SemaphoreType.DMA
    vmem = pl.BlockSpec(memory_space=pltpu.VMEM)
    hbm = pl.BlockSpec(memory_space=pltpu.HBM)
    x_shape = (HALVES, col_count, row_count, HALF_ROWS, points)
    operands = [occ, vir, occ_decay, vir_decay]
    in_specs = [hbm, hbm, vmem, vmem]
    scratch = [pltpu.VMEM((row_count, b, points), bf16) for b in bands]
    scratch += [pltpu.VMEM((outer, inner, b, window), bf16) for b in bands]
    scratch += [pltpu.VMEM((window, row_count * b), bf16) for b in bands]
    scratch += [
        pltpu.VMEM((HALVES, block_rows, points), f32),
        pltpu.VMEM((HALVES, row_count, HALF_ROWS, points), bf16),
        pltpu.VMEM((points, points), bf16),
    ]
    if fused:
        cosine, sine = plane_tables()
        line = line_tables(col_count)
        operands += [line, cosine, sine]
        in_specs += [hbm] * 3
        wide = (LANES // NB) * LANES
        scratch += [
            pltpu.VMEM(x_shape, bf16),
            pltpu.VMEM((wide, wide), bf16),
            pltpu.VMEM(line.shape[1:], bf16),
            pltpu.VMEM(cosine.shape, bf16),
            pltpu.VMEM(sine.shape, bf16),
            pltpu.VMEM((NC * R_BLOCK, (row_count // 2) * NB), bf16),
            dma((3,)),
        ]
        out = jax.ShapeDtypeStruct((HALVES * line.shape[1] // 2, NAB), f32)
        out_shape = [out, out]
    else:
        out_shape = [jax.ShapeDtypeStruct(x_shape, bf16)]
    scratch += [dma((2, parts, row_count))] * 2
    scratch += [dma((2, col_count))] * 2
    scratch += [dma((2, outer))] * 2
    scratch += [dma((2, inner, col_count))] * 2
    scratch += [dma((HALVES, row_count))] * 2
    scratch += [dma((HALVES, col_count, row_count))] * 2
    scratch += [dma((4,))]
    cfg = (row_count, col_count, inner, cuts, factor, fused)
    result = pl.pallas_call(
        functools.partial(whole_kernel, cfg),
        out_shape=out_shape,
        in_specs=in_specs,
        out_specs=[vmem] * len(out_shape),
        scratch_shapes=scratch,
        compiler_params=pltpu.CompilerParams(
            collective_id=0, has_side_effects=True, vmem_limit_bytes=52 * 1024 * 1024
        ),
    )(*operands)
    return fused, result


def on_device(rows_dev, occupied_waves, virtual_waves, occupied_decay, virtual_decay):
    row_count = lax.axis_size("row")
    col_count = lax.axis_size("col")
    nocc, nvir = occupied_decay.shape[0], virtual_decay.shape[0]
    window = rows_dev * row_count
    points = occupied_waves.shape[1] // row_count
    factor = -1.0 / math.sqrt(nocc * nvir) / math.sqrt(NGRID)
    fused, result = whole(
        row_count,
        col_count,
        occupied_waves,
        virtual_waves,
        occupied_decay.reshape(1, nocc),
        virtual_decay.reshape(1, nvir),
        window,
        factor,
    )
    if fused:
        real_part, imag_part = result
    else:
        x = result[0].reshape(HALVES, col_count * row_count, R_BLOCK, NC, points // NC)
        x = jnp.transpose(x, (3, 0, 2, 1, 4)).reshape(NC, rows_dev, NAB)
        real_part, imag_part = spectrum(x, line_tables(col_count))
    shape = (rows_dev, NC // col_count, NAB)
    return real_part.reshape(shape), imag_part.reshape(shape)


ROWS_DEV = 32


def solution(mesh):
    in_specs = (P("row", "col"), P("row", "col"), P(), P())
    out_specs = (P("row", "col", None), P("row", "col", None))
    return jax.shard_map(
        functools.partial(on_device, ROWS_DEV),
        mesh=mesh,
        in_specs=in_specs,
        out_specs=out_specs,
        check_vma=False,
    )
```

```python
import functools
import math

import jax
import jax.numpy as jnp
import numpy as np
from jax import lax
from jax.experimental import pallas as pl
from jax.experimental.pallas import tpu as pltpu
from jax.sharding import PartitionSpec as P

NA = 32
NB = 32
NC = 32
NAB = NA * NB
NGRID = NA * NB * NC
LANES = 128
R_BLOCK = 16


def trig(phase, length):
    angle = (phase % length) * (2.0 * math.pi / length)
    return np.cos(angle), np.sin(angle)


def bf16_table(table):
    return jnp.asarray(table.astype(np.float32)).astype(jnp.bfloat16)


def plane_tables():
    index = np.arange(NAB)
    a, b = index // NB, index % NB
    phase = a[:, None] * a[None, :] * NB + b[:, None] * b[None, :] * NA
    cosine, sine = trig(phase, NA * NB)
    return bf16_table(cosine), bf16_table(sine)


def line_tables(col_count):
    share = NC // col_count
    full = np.zeros((col_count, 2, R_BLOCK, share, NC, R_BLOCK))
    for y in range(col_count):
        kc = y * share + np.arange(share)
        cosine, sine = trig(kc[:, None] * np.arange(NC)[None, :], NC)
        for r in range(R_BLOCK):
            full[y, 0, r, :, :, r] = cosine
            full[y, 1, r, :, :, r] = -sine
    return bf16_table(full.reshape(col_count, 2 * R_BLOCK * share, NC * R_BLOCK))


def dot(a, b):
    return jnp.dot(a, b, preferred_element_type=jnp.float32)


def spectrum_kernel(x_ref, line_ref, cos_ref, sin_ref, re_ref, im_ref):
    rows = x_ref[...].reshape(NC * R_BLOCK, NAB)
    line = dot(line_ref[lax.axis_index("col")], rows).astype(jnp.bfloat16)
    half = line.shape[0] // 2
    re, im = line[:half], line[half:]
    re_ref[...] = dot(re, cos_ref[...]) + dot(im, sin_ref[...])
    im_ref[...] = dot(im, cos_ref[...]) - dot(re, sin_ref[...])


def spectrum(x, line_table):
    r_count = x.shape[1]
    cosine, sine = plane_tables()
    out_rows = line_table.shape[1] // 2
    steps = r_count // R_BLOCK
    whole = lambda table: pl.BlockSpec(table.shape, lambda i: (0,) * table.ndim)
    out = jax.ShapeDtypeStruct((out_rows * steps, NAB), jnp.float32)
    out_spec = pl.BlockSpec((out_rows, NAB), lambda i: (i, 0))
    return pl.pallas_call(
        spectrum_kernel,
        grid=(steps,),
        in_specs=[
            pl.BlockSpec((x.shape[0], R_BLOCK, x.shape[2]), lambda i: (0, i, 0)),
            whole(line_table),
            whole(cosine),
            whole(sine),
        ],
        out_specs=[out_spec, out_spec],
        out_shape=[out, out],
        compiler_params=pltpu.CompilerParams(vmem_limit_bytes=48 * 1024 * 1024),
    )(x, line_table, cosine, sine)


MESH = pl.DeviceIdType.MESH
HALVES = 2
VMEM_LIMIT = 47 * 1024 * 1024
PIECES = 4
FARS = 4
HALF_ROWS = R_BLOCK


def flip(index, mask):
    bits = [1 << bit for bit in range(mask.bit_length()) if mask >> bit & 1]
    for bit in bits:
        index = index + bit - 2 * bit * lax.rem(lax.div(index, bit), 2)
    return index


def group_size(row_count):
    return 4 if row_count % 4 == 0 else 1


def send(src, dst, send_sem, recv_sem, target):
    return pltpu.make_async_remote_copy(
        src_ref=src,
        dst_ref=dst,
        send_sem=send_sem,
        recv_sem=recv_sem,
        device_id=target,
        device_id_type=MESH,
    )


def drain(ref, sem):
    pltpu.make_async_copy(ref, ref, sem).wait()


def enter(row_count, col_count, inner, row, col):
    barrier = pltpu.get_barrier_semaphore()
    targets = [(flip(row, k), col) for k in range(1, row_count)]
    targets += [
        (flip(row, s), lax.rem(col + d, col_count))
        for d in range(1, col_count)
        for s in range(inner)
    ]
    for target in targets:
        pl.semaphore_signal(barrier, inc=1, device_id=target, device_id_type=MESH)
    return barrier, len(targets)


def fill(ref, values, rows):
    width = ref.shape[1]

    def step(i, carry):
        start = pl.multiple_of(i * rows, rows)
        row = lax.broadcasted_iota(jnp.int32, (rows, width), 0) + start
        lane = lax.broadcasted_iota(jnp.int32, (rows, width), 1)
        ref[pl.ds(start, rows), :] = jnp.where(values(row, lane), 1.0, 0.0).astype(jnp.bfloat16)
        return carry

    lax.fori_loop(0, ref.shape[0] // rows, step, 0)


def spread(blocks, swap, lines_buf, line_table):
    per = LANES // NB
    for g in range(len(blocks) // per):
        pieces = []
        for t in range(NC // per):
            lanes = pl.ds(t * LANES, LANES)
            pieces.append(jnp.concatenate([blocks[g * per + k][:, lanes] for k in range(per)], axis=1))
        moved = dot(jnp.concatenate(pieces, axis=0), swap[...]).astype(jnp.bfloat16)
        for t in range(NC // per):
            for j in range(per):
                lines_buf[pl.ds((t * per + j) * R_BLOCK, R_BLOCK), pl.ds(g * LANES, LANES)] = moved[
                    t * R_BLOCK : (t + 1) * R_BLOCK, j * LANES : (j + 1) * LANES
                ]
    line = dot(line_table[...], lines_buf[...]).astype(jnp.bfloat16)
    half = line.shape[0] // 2
    return line[:half], line[half:]


def whole_kernel(cfg, *refs):
    (row_count, col_count, inner, cuts, factor, fused) = cfg
    refs = list(refs)
    take = lambda n: [refs.pop(0) for _ in range(n)]
    occ_ref, vir_ref, occ_decay, vir_decay = take(4)
    if fused:
        (table_hbm,) = take(1)
        parts_out = take(2 * PIECES)
        tail_x, tail_cos, tail_sin, tail_line, tail_swap = take(5)
    else:
        (x_ref,) = take(1)
    planes = take(2)
    raws = take(2)
    lefts = take(2)
    mixed, polar, swap = take(3)
    if fused:
        x_ref, piece_swap, line_ref, cos_ref, sin_ref, lines_buf, acc_re, acc_im = take(8)
        table_sem, out_sem, tail_sem = take(3)
    (wave_send, wave_recv, col_send, col_recv, line_send, line_recv, share_send, share_recv) = take(8)
    (give_send, give_recv, pass_send, pass_recv, local) = take(5)

    row, col = lax.axis_index("row"), lax.axis_index("col")
    outer = row_count // inner
    mine, seat = lax.div(row, inner), lax.rem(row, inner)
    points = occ_ref.shape[1] // row_count
    waves = (occ_ref, vir_ref)
    window = raws[0].shape[3]
    share = window // col_count
    block_rows = row_count * HALF_ROWS

    def peer(k):
        return flip(row, k)

    barrier, arrivals = enter(row_count, col_count, inner, row, col)

    own = []
    for i in range(2):
        lanes = pl.ds(pl.multiple_of(row * points, LANES), points)
        own.append(pltpu.make_async_copy(waves[i].at[:, lanes], planes[i].at[row], local.at[i]))
    if fused:
        width = line_ref.shape[0]
        lines = pl.ds(pl.multiple_of(2 * NAB + col * width, width), width)
        own.append(pltpu.make_async_copy(table_hbm.at[lines, pl.ds(0, width)], line_ref, table_sem.at[0]))
        own.append(pltpu.make_async_copy(table_hbm.at[pl.ds(0, NAB)], cos_ref, table_sem.at[1]))
        own.append(pltpu.make_async_copy(table_hbm.at[pl.ds(NAB, NAB)], sin_ref, table_sem.at[2]))
    for copy in own:
        copy.start()
    pl.semaphore_wait(barrier, arrivals)

    def start_waves(part, ks):
        first, last = cuts[part], cuts[part + 1]
        for k in ks:
            to = peer(k)
            lanes = pl.ds(pl.multiple_of(to * points + first, LANES), last - first)
            for i in range(2):
                copy = send(
                    waves[i].at[:, lanes],
                    planes[i].at[row, :, pl.ds(first, last - first)],
                    wave_send.at[i],
                    wave_recv.at[i, part],
                    (to, col),
                )
                copy.start()

    def wait_waves(part):
        lanes = pl.ds(cuts[part], cuts[part + 1] - cuts[part])
        for i in range(2):
            drain(planes[i].at[pl.ds(0, row_count - 1), :, lanes], wave_recv.at[i, part])

    parts = len(cuts) - 1
    near = row_count // 2

    def slab_share(c):
        return pl.ds(c * share, share) if isinstance(c, int) else pl.ds(pl.multiple_of(c * share, LANES), share)

    def over_col(i, c):
        return send(
            waves[i].at[:, slab_share(c)],
            raws[i].at[mine, seat, :, slab_share(c)],
            col_send.at[i, c - 1],
            col_recv.at[i],
            (row, c),
        )

    @pl.when(col == 0)
    def _():
        for i in range(2):
            for c in range(1, col_count):
                over_col(i, c).start()
            pltpu.make_async_copy(
                waves[i].at[:, slab_share(0)], raws[i].at[mine, seat, :, slab_share(0)], local.at[2 + i]
            ).start()

    far = range(near, row_count)
    queue = [k for s in range(inner) for k in far if k % inner == s]
    queue += [k for k in range(inner, near)] + [k for k in range(1, inner)]

    def advance(count):
        start_waves(0, queue[:count])
        del queue[:count]

    advance(1)

    @pl.when(col == 0)
    def _():
        for i in range(2):
            pltpu.make_async_copy(
                waves[i].at[:, slab_share(0)], raws[i].at[mine, seat, :, slab_share(0)], local.at[2 + i]
            ).wait()

    if col_count > 1:

        @pl.when(col != 0)
        def _():
            for i in range(2):
                over_col(i, 1).wait_recv()

    sent = []
    mine, seat = lax.div(row, inner), lax.rem(row, inner)

    def exchange(pairs):
        started = [send(place, place, line_send.at[i, n], line_recv.at[i, n], to) for i, n, place, to in pairs]
        for copy in started:
            copy.start()
        sent.extend(started)
        return started

    held = [0]
    number = 0
    for bit in [1 << bit for bit in reversed(range((outer - 1).bit_length()))]:
        to = (flip(row, bit * inner), col)
        started = exchange(
            [
                (i, number + n, raws[i].at[flip(mine, mask), seat, :, slab_share(col)], to)
                for n, mask in enumerate(held)
                for i in range(2)
            ]
        )
        number += len(held)
        held = held + [mask + bit for mask in held]
        advance(1)
        for copy in started:
            copy.wait_recv()
    started = []
    for d in range(1, col_count):
        for i in range(2):
            place = raws[i].at[:, seat, :, slab_share(col)]
            to = (row, lax.rem(col + d, col_count))
            started.append(send(place, place, share_send.at[i, d - 1], share_recv.at[i, d - 1], to))
    for copy in started:
        copy.start()
    sent.extend(started)
    advance(1)
    for copy in started:
        copy.wait_recv()
    held = [0]
    for bit in [1 << bit for bit in reversed(range((inner - 1).bit_length()))]:
        to = (flip(row, bit), col)
        started = exchange(
            [
                (i, number + n, raws[i].at[:, flip(seat, mask)], to)
                for n, mask in enumerate(held)
                for i in range(2)
            ]
        )
        number += len(held)
        held = held + [mask + bit for mask in held]
        advance(2)
        for copy in started:
            copy.wait_recv()
    advance(len(queue))
    order = [k for k in far] + [k for k in range(inner, near)] + [k for k in range(1, inner)]
    for part in range(1, parts):
        start_waves(part, order)

    per_point = points // NC
    fill(swap, lambda p, n: n == (p & (NC - 1)) * per_point + lax.div(p, NC), min(LANES, points))
    if fused:
        per = LANES // NB
        inside = per * NB

        def piece(p, n):
            k, j, w = lax.div(p, inside), lax.div(p & (inside - 1), NB), p & (NB - 1)
            return n == j * inside + k * NB + w

        fill(piece_swap, piece, LANES)
        acc_re[...] = jnp.zeros_like(acc_re)
        acc_im[...] = jnp.zeros_like(acc_im)

    for i, decay in enumerate((occ_decay, vir_decay)):
        raw, left = raws[i], lefts[i]
        bands = raw.shape[2]
        join = max(1, LANES // (inner * bands))
        width = join * inner * bands

        def scale(m, carry, raw=raw, left=left, decay=decay, width=width, join=join):
            lanes = pl.ds(pl.multiple_of(m * width, width), width)
            factors = decay[:, lanes]
            for t in range(window // LANES):
                piece = raw[pl.ds(m * join, join), :, :, pl.ds(t * LANES, LANES)]
                turned = piece.reshape(width, LANES).astype(jnp.float32).T * factors
                turned = turned.astype(jnp.bfloat16)
                for s in range(LANES // HALF_ROWS):
                    q = (t * LANES + s * HALF_ROWS) // (HALVES * HALF_ROWS)
                    at = ((s % HALVES) * row_count + q) * HALF_ROWS
                    left[pl.ds(at, HALF_ROWS), lanes] = turned[s * HALF_ROWS : (s + 1) * HALF_ROWS]
            return carry

        lax.fori_loop(0, outer // join, scale, 0)

    def product(h, first, width):
        rows = pl.ds(h * block_rows, block_rows)
        lanes = pl.ds(first, width)
        green = []
        for i in range(2):
            wave = planes[i][:, :, lanes]
            wave = wave.reshape(wave.shape[0] * wave.shape[1], width)
            green.append(dot(lefts[i][rows, :], wave))
        value = (green[0] * green[1] * factor).astype(jnp.bfloat16)
        return dot(value, swap[lanes, :])

    for copy in own[:2]:
        copy.wait()
    ordered = [k for s in range(inner) for k in far if k % inner == s]
    quarter = len(ordered) // FARS
    fars = [ordered[n * quarter : (n + 1) * quarter] for n in range(FARS)]
    keep = []

    def to_row(h, ks, group):
        for k in ks:
            send(
                polar.at[h, peer(k)],
                x_ref.at[h, col, row],
                give_send.at[h],
                give_recv.at[h, group],
                (peer(k), col),
            ).start()

    def to_cols(h, ks):
        for k in ks:
            for d in range(1, col_count):
                send(
                    polar.at[h, peer(k)],
                    x_ref.at[h, col, row],
                    pass_send.at[h],
                    pass_recv.at[h, d - 1, 0],
                    (peer(k), lax.rem(col + d, col_count)),
                ).start()

    def forward(h, group):
        some = fars[group]
        drain(x_ref.at[h, col, pl.ds(0, len(some))], give_recv.at[h, 1 + group])
        for k in some:
            arrived = x_ref.at[h, col, peer(k)]
            for d in range(1, col_count):
                slot = arrived
                if fused and h == HALVES - 1:
                    slot = tail_x.at[d - 1, lax.rem(peer(k), near)]
                to = (row, lax.rem(col + d, col_count))
                send(arrived, slot, pass_send.at[h], pass_recv.at[h, d - 1, 1], to).start()

    def wait_near(h):
        drain(x_ref.at[h, col, pl.ds(0, near - 1)], give_recv.at[h, 0])
        keep[h].wait()

    def wait_pass(h, which):
        for d in range(1, col_count):
            count = row_count - near if which else near
            drain(x_ref.at[h, col, pl.ds(0, count)], pass_recv.at[h, d - 1, which])

    def give(h):
        copy = pltpu.make_async_copy(polar.at[h, row], x_ref.at[h, col, row], local.at[2 + h])
        copy.start()
        keep.append(copy)
        to_cols(h, range(min(2, inner)))
        for group in range(FARS):
            to_row(h, fars[group], 1 + group)
        to_row(h, range(inner, near), 0)
        to_row(h, range(1, inner), 0)
        to_cols(h, range(min(2, inner), near))

    for part in range(parts):
        wait_waves(part)
        first, last = cuts[part], cuts[part + 1]
        tile = min(last - first, 2 * LANES)
        for h in range(HALVES):
            moved = mixed[h] if part else None
            for start in range(first, last, tile):
                term = product(h, start, tile)
                moved = term if moved is None else moved + term
            if part < parts - 1:
                mixed[h] = moved
            else:
                polar[h] = moved.astype(jnp.bfloat16).reshape(row_count, HALF_ROWS, points)
                give(h)

    if fused:
        for copy in own[2:]:
            copy.wait()
        per = LANES // NB
        side = lax.div(row, near)
        other = 1 - side

        wide = near * NB
        tails = [
            pltpu.make_async_copy(line_ref, tail_line, tail_sem.at[0]),
            pltpu.make_async_copy(piece_swap, tail_swap, tail_sem.at[1]),
        ]
        for d in range(1, col_count):
            c = lax.rem(col + col_count - d, col_count)
            depth = pl.ds(pl.multiple_of((c * 2 + other) * wide, wide), wide)
            tails.append(pltpu.make_async_copy(cos_ref.at[depth], tail_cos.at[d - 1], tail_sem.at[2 * d]))
            tails.append(pltpu.make_async_copy(sin_ref.at[depth], tail_sin.at[d - 1], tail_sem.at[2 * d + 1]))
        for copy in tails:
            copy.start()

        def transform(h, c, z):
            blocks = [x_ref.at[h, c, z * near + a] for a in range(near)]
            re, im = spread(blocks, piece_swap, lines_buf, line_ref)
            depth = pl.ds(pl.multiple_of((c * 2 + z) * wide, wide), wide)
            cosine, sine = cos_ref[depth, :], sin_ref[depth, :]
            acc_re[h] += dot(re, cosine) + dot(im, sine)
            acc_im[h] += dot(im, cosine) - dot(re, sine)

        def put_out(h):
            per_half = PIECES // HALVES
            height = acc_re.shape[1] // per_half
            for i, acc in enumerate((acc_re, acc_im)):
                for n in range(per_half):
                    p = i * PIECES + h * per_half + n
                    pltpu.make_async_copy(
                        acc.at[h, pl.ds(n * height, height)], parts_out[p], out_sem.at[h]
                    ).start()

    else:
        side = other = 0

        def transform(h, c, z):
            return

        def put_out(h):
            return

        tails = []
    others = [lax.rem(col + d, col_count) for d in range(1, col_count)]
    forward(0, 0)
    forward(0, 1)
    wait_near(0)
    transform(0, col, side)
    forward(0, 2)
    forward(0, 3)
    wait_pass(0, 0)
    for c in others:
        transform(0, c, side)
    transform(0, col, other)
    forward(1, 0)
    forward(1, 1)
    wait_near(1)
    transform(1, col, side)
    forward(1, 2)
    wait_pass(0, 1)
    for c in others:
        transform(0, c, other)
    put_out(0)
    wait_pass(1, 0)
    for c in others:
        transform(1, c, side)
    forward(1, 3)
    transform(1, col, other)
    put_out(1)
    wait_pass(1, 1)
    for copy in tails:
        copy.wait()
    if fused:
        for h in range(HALVES):
            drain(acc_re, out_sem.at[h])

    for i in range(2):
        drain(planes[i].at[pl.ds(0, row_count - 1)], wave_send.at[i])
    for copy in sent:
        copy.wait_send()
    for h in range(HALVES):
        drain(x_ref.at[h, col, pl.ds(0, row_count - 1)], give_send.at[h])
        for d in range(1, col_count):
            drain(x_ref.at[h, col], pass_send.at[h])

    @pl.when(col == 0)
    def _():
        for i in range(2):
            for c in range(1, col_count):
                over_col(i, c).wait_send()

    if not fused:
        for copy in own[2:]:
            copy.wait()


def whole(row_count, col_count, occ, vir, occ_decay, vir_decay, window, factor):
    inner = group_size(row_count)
    outer = row_count // inner
    points = occ.shape[1] // row_count
    fused = points == NB * NC and row_count * col_count == NA and (row_count // 2) % (LANES // NB) == 0
    quarter = points // 4
    cuts = (0, points - quarter, points) if quarter % LANES == 0 else (0, points)
    parts = len(cuts) - 1
    bands = (occ.shape[0], vir.shape[0])
    block_rows = row_count * HALF_ROWS
    bf16, f32 = jnp.bfloat16, jnp.float32
    dma = pltpu.SemaphoreType.DMA
    vmem = pl.BlockSpec(memory_space=pltpu.VMEM)
    hbm = pl.BlockSpec(memory_space=pltpu.HBM)
    x_shape = (HALVES, col_count, row_count, HALF_ROWS, points)
    operands = [occ, vir, occ_decay, vir_decay]
    in_specs = [hbm, hbm, vmem, vmem]
    scratch = [pltpu.VMEM((row_count, b, points), bf16) for b in bands]
    scratch += [pltpu.VMEM((outer, inner, b, window), bf16) for b in bands]
    scratch += [pltpu.VMEM((window, row_count * b), bf16) for b in bands]
    scratch += [
        pltpu.VMEM((HALVES, block_rows, points), f32),
        pltpu.VMEM((HALVES, row_count, HALF_ROWS, points), bf16),
        pltpu.VMEM((points, points), bf16),
    ]
    if fused:
        cosine, sine = plane_tables()
        line = line_tables(col_count)
        flat = jnp.pad(line.reshape(-1, line.shape[2]), ((0, 0), (0, NAB - line.shape[2])))
        operands += [jnp.concatenate([cosine, sine, flat])]
        in_specs += [hbm]
        wide = (LANES // NB) * LANES
        scratch += [
            pltpu.VMEM(x_shape, bf16),
            pltpu.VMEM((wide, wide), bf16),
            pltpu.VMEM(line.shape[1:], bf16),
            pltpu.VMEM(cosine.shape, bf16),
            pltpu.VMEM(sine.shape, bf16),
            pltpu.VMEM((NC * R_BLOCK, (row_count // 2) * NB), bf16),
        ]
        scratch += [pltpu.VMEM((HALVES, line.shape[1] // 2, NAB), f32)] * 2
        scratch += [dma((3,)), dma((HALVES,)), dma((2 * col_count,))]
        out_shape = [jax.ShapeDtypeStruct((HALVES * line.shape[1] // 2 // PIECES, NAB), f32)] * (2 * PIECES)
        late = col_count - 1
        near = row_count // 2
        tails = [(late, near, HALF_ROWS, points)] + [(late, near * NB, NAB)] * 2 + [line.shape[1:], (wide, wide)]
        out_shape += [jax.ShapeDtypeStruct(shape, bf16) for shape in tails]
    else:
        out_shape = [jax.ShapeDtypeStruct(x_shape, bf16)]
    places = max(1, col_count - 1)
    steps = outer - 1 + inner - 1
    scratch += [dma((2,)), dma((2, parts)), dma((2, places)), dma((2,))]
    scratch += [dma((2, steps))] * 2 + [dma((2, places))] * 2
    scratch += [dma((HALVES,)), dma((HALVES, 1 + FARS)), dma((HALVES,)), dma((HALVES, places, 2))]
    scratch += [dma((4,))]
    cfg = (row_count, col_count, inner, cuts, factor, fused)
    result = pl.pallas_call(
        functools.partial(whole_kernel, cfg),
        out_shape=out_shape,
        in_specs=in_specs,
        out_specs=[pl.BlockSpec(memory_space=pl.ANY) if fused else vmem] * len(out_shape),
        scratch_shapes=scratch,
        compiler_params=pltpu.CompilerParams(
            collective_id=0, has_side_effects=True, vmem_limit_bytes=VMEM_LIMIT
        ),
    )(*operands)
    return fused, result


def last_kernel(*refs):
    parts = refs[: 2 * PIECES]
    tail_x, tail_cos, tail_sin, tail_line, tail_swap, re_out, im_out, lines_buf, *acc, sems = refs[2 * PIECES :]
    outs = (re_out, im_out)
    half = PIECES // HALVES
    rows = parts[0].shape[0]
    copies = []

    def put(i, p, src):
        copy = pltpu.make_async_copy(src, outs[i].at[pl.ds(p * rows, rows)], sems.at[i, p])
        copy.start()
        copies.append(copy)

    for i in range(2):
        for p in range(half):
            put(i, p, parts[i * PIECES + p])
    late = []
    for d in range(tail_x.shape[0]):
        blocks = [tail_x.at[d, a] for a in range(tail_x.shape[1])]
        re, im = spread(blocks, tail_swap, lines_buf, tail_line)
        late.append((re, im, tail_cos[d], tail_sin[d]))
    for n in range(half):
        p = half + n
        at = slice(n * rows, (n + 1) * rows)
        for i in range(2):
            total = parts[i * PIECES + p][...]
            for re, im, cosine, sine in late:
                if i == 0:
                    total = total + (dot(re[at], cosine) + dot(im[at], sine))
                else:
                    total = total + (dot(im[at], cosine) - dot(re[at], sine))
            acc[i][pl.ds(n * rows, rows), :] = total
            put(i, p, acc[i].at[pl.ds(n * rows, rows)])
    for copy in copies:
        copy.wait()


def last(operands):
    rows, lanes = operands[0].shape
    vmem = pl.BlockSpec(memory_space=pltpu.VMEM)
    tail_x = operands[2 * PIECES]
    acc = pltpu.VMEM((rows * PIECES // HALVES, lanes), jnp.float32)
    return pl.pallas_call(
        last_kernel,
        out_shape=[jax.ShapeDtypeStruct((rows * PIECES, lanes), jnp.float32)] * 2,
        in_specs=[vmem] * len(operands),
        out_specs=[pl.BlockSpec(memory_space=pltpu.HBM)] * 2,
        scratch_shapes=[
            pltpu.VMEM((NC * R_BLOCK, tail_x.shape[1] * NB), jnp.bfloat16),
            acc,
            acc,
            pltpu.SemaphoreType.DMA((2, PIECES)),
        ],
        compiler_params=pltpu.CompilerParams(vmem_limit_bytes=8 * 1024 * 1024),
    )(*operands)


def on_device(rows_dev, occupied_waves, virtual_waves, occupied_decay, virtual_decay):
    row_count = lax.axis_size("row")
    col_count = lax.axis_size("col")
    nocc, nvir = occupied_decay.shape[0], virtual_decay.shape[0]
    window = rows_dev * row_count
    points = occupied_waves.shape[1] // row_count
    factor = -1.0 / math.sqrt(nocc * nvir) / math.sqrt(NGRID)
    fused, result = whole(
        row_count,
        col_count,
        occupied_waves,
        virtual_waves,
        occupied_decay.reshape(1, nocc),
        virtual_decay.reshape(1, nvir),
        window,
        factor,
    )
    if fused:
        real_part, imag_part = last(result)
    else:
        x = result[0].reshape(HALVES, col_count * row_count, R_BLOCK, NC, points // NC)
        x = jnp.transpose(x, (3, 0, 2, 1, 4)).reshape(NC, rows_dev, NAB)
        real_part, imag_part = spectrum(x, line_tables(col_count))
    shape = (rows_dev, NC // col_count, NAB)
    return real_part.reshape(shape), imag_part.reshape(shape)


ROWS_DEV = 32


def solution(mesh):
    in_specs = (P("row", "col"), P("row", "col"), P(), P())
    out_specs = (P("row", "col", None), P("row", "col", None))
    return jax.shard_map(
        functools.partial(on_device, ROWS_DEV),
        mesh=mesh,
        in_specs=in_specs,
        out_specs=out_specs,
        check_vma=False,
    )
```

```python
import functools
import math

import jax
import jax.numpy as jnp
import numpy as np
from jax import lax
from jax.experimental import pallas as pl
from jax.experimental.pallas import tpu as pltpu
from jax.sharding import PartitionSpec as P

NA = 32
NB = 32
NC = 32
NAB = NA * NB
NGRID = NA * NB * NC
LANES = 128
R_BLOCK = 16


def trig(phase, length):
    angle = (phase % length) * (2.0 * math.pi / length)
    return np.cos(angle), np.sin(angle)


def bf16_table(table):
    return jnp.asarray(table.astype(np.float32)).astype(jnp.bfloat16)


def plane_tables(turns, group):
    index = np.arange(NAB)
    a, b = index // NB, index % NB
    phase = a[:, None] * a[None, :] * NB + b[:, None] * b[None, :] * NA
    rows = index.reshape(-1, group // turns, turns, NB).transpose(0, 2, 1, 3).reshape(-1)
    cosine, sine = trig(phase[rows], NA * NB)
    return bf16_table(cosine), bf16_table(sine)


def line_tables(col_count):
    share = NC // col_count
    full = np.zeros((col_count, 2, R_BLOCK, share, NC, R_BLOCK))
    for y in range(col_count):
        kc = y * share + np.arange(share)
        cosine, sine = trig(kc[:, None] * np.arange(NC)[None, :], NC)
        for r in range(R_BLOCK):
            full[y, 0, r, :, :, r] = cosine
            full[y, 1, r, :, :, r] = -sine
    return bf16_table(full.reshape(col_count, 2 * R_BLOCK * share, NC * R_BLOCK))


def dot(a, b):
    return jnp.dot(a, b, preferred_element_type=jnp.float32)


def spectrum_kernel(x_ref, line_ref, cos_ref, sin_ref, re_ref, im_ref):
    rows = x_ref[...].reshape(NC * R_BLOCK, NAB)
    line = dot(line_ref[lax.axis_index("col")], rows).astype(jnp.bfloat16)
    half = line.shape[0] // 2
    re, im = line[:half], line[half:]
    re_ref[...] = dot(re, cos_ref[...]) + dot(im, sin_ref[...])
    im_ref[...] = dot(im, cos_ref[...]) - dot(re, sin_ref[...])


def spectrum(x, line_table):
    r_count = x.shape[1]
    cosine, sine = plane_tables(1, NA)
    out_rows = line_table.shape[1] // 2
    steps = r_count // R_BLOCK
    whole = lambda table: pl.BlockSpec(table.shape, lambda i: (0,) * table.ndim)
    out = jax.ShapeDtypeStruct((out_rows * steps, NAB), jnp.float32)
    out_spec = pl.BlockSpec((out_rows, NAB), lambda i: (i, 0))
    return pl.pallas_call(
        spectrum_kernel,
        grid=(steps,),
        in_specs=[
            pl.BlockSpec((x.shape[0], R_BLOCK, x.shape[2]), lambda i: (0, i, 0)),
            whole(line_table),
            whole(cosine),
            whole(sine),
        ],
        out_specs=[out_spec, out_spec],
        out_shape=[out, out],
        compiler_params=pltpu.CompilerParams(vmem_limit_bytes=48 * 1024 * 1024),
    )(x, line_table, cosine, sine)


MESH = pl.DeviceIdType.MESH
HALVES = 2
VMEM_LIMIT = 48 * 1024 * 1024
PIECES = 4
FARS = 4
AHEAD = (1, 2, 1)
HALF_ROWS = R_BLOCK


def flip(index, mask):
    bits = [1 << bit for bit in range(mask.bit_length()) if mask >> bit & 1]
    for bit in bits:
        index = index + bit - 2 * bit * lax.rem(lax.div(index, bit), 2)
    return index


def group_size(row_count):
    return 4 if row_count % 4 == 0 else 1


def send(src, dst, send_sem, recv_sem, target):
    return pltpu.make_async_remote_copy(
        src_ref=src,
        dst_ref=dst,
        send_sem=send_sem,
        recv_sem=recv_sem,
        device_id=target,
        device_id_type=MESH,
    )


def drain(ref, sem):
    pltpu.make_async_copy(ref, ref, sem).wait()


def enter(row_count, col_count, inner, row, col):
    barrier = pltpu.get_barrier_semaphore()
    targets = [(flip(row, k), col) for k in range(1, row_count)]
    targets += [
        (flip(row, s), lax.rem(col + d, col_count))
        for d in range(1, col_count)
        for s in range(inner)
    ]
    for target in targets:
        pl.semaphore_signal(barrier, inc=1, device_id=target, device_id_type=MESH)
    return barrier, len(targets)


def fill(ref, values, rows):
    width = ref.shape[1]

    def step(i, carry):
        start = pl.multiple_of(i * rows, rows)
        row = lax.broadcasted_iota(jnp.int32, (rows, width), 0) + start
        lane = lax.broadcasted_iota(jnp.int32, (rows, width), 1)
        ref[pl.ds(start, rows), :] = jnp.where(values(row, lane), 1.0, 0.0).astype(jnp.bfloat16)
        return carry

    lax.fori_loop(0, ref.shape[0] // rows, step, 0)


def spread(blocks, lines_buf, line_table):
    short = blocks[0].shape[1] // NC
    per = LANES // short
    count = blocks[0].shape[1] // LANES
    groups = len(blocks) // per
    pieces = []
    for k in range(per):
        parts = [blocks[g * per + k][:, pl.ds(t * LANES, LANES)] for g in range(groups) for t in range(count)]
        pieces.append(jnp.concatenate(parts, axis=0))
    lane = lax.broadcasted_iota(jnp.int32, pieces[0].shape, 1)
    bit = per // 2
    while bit:
        high = (lane & (bit * short)) != 0
        for k in range(per):
            if k & bit:
                continue
            a, b = pieces[k], pieces[k + bit]
            pieces[k] = jnp.where(high, pltpu.roll(b, bit * short, 1), a)
            pieces[k + bit] = jnp.where(high, b, pltpu.roll(a, LANES - bit * short, 1))
        bit //= 2
    for g in range(groups):
        for t in range(count):
            at = (g * count + t) * R_BLOCK
            for j in range(per):
                place = pl.ds((t * per + j) * R_BLOCK, R_BLOCK)
                lines_buf[place, pl.ds(g * LANES, LANES)] = pieces[j][at : at + R_BLOCK]
    line = dot(line_table[...], lines_buf[...]).astype(jnp.bfloat16)
    half = line.shape[0] // 2
    re, im = line[:half], line[half:]
    return jnp.concatenate([jnp.concatenate([re, im], axis=1), jnp.concatenate([im, -re], axis=1)], axis=0)


def whole_kernel(cfg, *refs):
    (row_count, col_count, inner, turns, parts, factor, fused) = cfg
    refs = list(refs)
    take = lambda n: [refs.pop(0) for _ in range(n)]
    occ_ref, vir_ref, decays = take(3)
    if fused:
        (table_hbm,) = take(1)
        parts_out = take(2 * PIECES)
        tail_x, tail_cos, tail_sin, tail_line = take(4)
    else:
        (x_ref,) = take(1)
    planes = take(2)
    raws = take(2)
    lefts = take(2)
    mixed, polar, swap = take(3)
    if fused:
        x_ref, line_ref, plane_ref, lines_buf, acc_ref = take(5)
        table_sem, out_sem, tail_sem = take(3)
    (wave_send, wave_recv, col_send, col_recv, line_send, line_recv, share_send, share_recv) = take(8)
    (give_send, give_recv, pass_send, pass_recv, local, col_local, keep_sem) = take(7)

    row, col = lax.axis_index("row"), lax.axis_index("col")
    outer = row_count // inner
    mine, seat = lax.div(row, inner), lax.rem(row, inner)
    points = occ_ref.shape[1] // row_count
    waves = (occ_ref, vir_ref)
    window = raws[0].shape[3]
    share = window // col_count
    block_rows = row_count * HALF_ROWS

    def peer(k):
        return flip(row, k)

    barrier, arrivals = enter(row_count, col_count, inner, row, col)

    own = []
    span = points // turns

    def share_of(to, turn):
        return (lax.div(to, turns) * turns + turn) * points + lax.rem(to, turns) * span

    for turn in range(turns):
        for i in range(2):
            lanes = pl.ds(pl.multiple_of(share_of(row, turn), LANES), span)
            place = planes[i].at[row, :, pl.ds(turn * span, span)]
            own.append(pltpu.make_async_copy(waves[i].at[:, lanes], place, local.at[turn, i]))
    if fused:
        width = line_ref.shape[0]
        lines = pl.ds(pl.multiple_of(2 * NAB + col * width, width), width)
        own.append(pltpu.make_async_copy(table_hbm.at[lines, pl.ds(0, width)], line_ref, table_sem.at[0]))
        own.append(pltpu.make_async_copy(table_hbm.at[pl.ds(0, 2 * NAB)], plane_ref, table_sem.at[1]))
    for copy in own:
        copy.start()
    pl.semaphore_wait(barrier, arrivals)

    def start_waves(part, ks):
        turn, first, last = parts[part]
        for k in ks:
            to = peer(k)
            lanes = pl.ds(pl.multiple_of(share_of(to, turn) + first, LANES), last - first)
            for i in range(2):
                copy = send(
                    waves[i].at[:, lanes],
                    planes[i].at[row, :, pl.ds(turn * span + first, last - first)],
                    wave_send.at[i],
                    wave_recv.at[i, part],
                    (to, col),
                )
                copy.start()

    def wait_waves(part):
        turn, first, last = parts[part]
        lanes = pl.ds(turn * span + first, last - first)
        for i in range(2):
            drain(planes[i].at[pl.ds(0, row_count - 1), :, lanes], wave_recv.at[i, part])

    near = row_count // 2

    def slab_share(c):
        return pl.ds(c * share, share) if isinstance(c, int) else pl.ds(pl.multiple_of(c * share, LANES), share)

    def over_col(i, c):
        return send(
            waves[i].at[:, slab_share(c)],
            raws[i].at[mine, seat, :, slab_share(c)],
            col_send.at[i, c - 1],
            col_recv.at[i],
            (row, c),
        )

    @pl.when(col == 0)
    def _():
        for i in range(2):
            for c in range(1, col_count):
                over_col(i, c).start()
            pltpu.make_async_copy(
                waves[i].at[:, slab_share(0)], raws[i].at[mine, seat, :, slab_share(0)], col_local.at[i]
            ).start()

    far = range(near, row_count)
    seats = [[k for k in far if k % inner == s] for s in range(inner)]
    count = len(parts)
    middle = inner // 2
    near_all = list(range(inner, near)) + list(range(1, inner))
    far_straight = [k for ks in seats[:middle] for k in ks]
    far_turned = [k for ks in seats[middle:] for k in ks]
    straight = [(part, k) for part in range(count) for k in far_straight]
    turned = [(part, k) for part in range(count) for k in far_turned]

    def advance(some):
        for part, k in some:
            start_waves(part, [k])

    def ahead(count):
        advance(straight[:count])
        del straight[:count]

    ahead(1)

    @pl.when(col == 0)
    def _():
        for i in range(2):
            pltpu.make_async_copy(
                waves[i].at[:, slab_share(0)], raws[i].at[mine, seat, :, slab_share(0)], col_local.at[i]
            ).wait()

    if col_count > 1:

        @pl.when(col != 0)
        def _():
            for i in range(2):
                over_col(i, 1).wait_recv()

    sent = []
    mine, seat = lax.div(row, inner), lax.rem(row, inner)

    def exchange(pairs):
        started = [send(place, place, line_send.at[i, n], line_recv.at[i, n], to) for i, n, place, to in pairs]
        for copy in started:
            copy.start()
        sent.extend(started)
        return started

    held = [0]
    number = 0
    for bit in [1 << bit for bit in reversed(range((outer - 1).bit_length()))]:
        to = (flip(row, bit * inner), col)
        started = exchange(
            [
                (i, number + n, raws[i].at[flip(mine, mask), seat, :, slab_share(col)], to)
                for n, mask in enumerate(held)
                for i in range(2)
            ]
        )
        number += len(held)
        held = held + [mask + bit for mask in held]
        ahead(AHEAD[0] if bit * 2 >= outer else AHEAD[1])
        for copy in started:
            copy.wait_recv()
    started = []
    for d in range(1, col_count):
        for i in range(2):
            place = raws[i].at[:, seat, :, slab_share(col)]
            to = (row, lax.rem(col + d, col_count))
            started.append(send(place, place, share_send.at[i, d - 1], share_recv.at[i, d - 1], to))
    for copy in started:
        copy.start()
    sent.extend(started)
    ahead(AHEAD[2])
    for copy in started:
        copy.wait_recv()
    held = [0]
    for bit in [1 << bit for bit in reversed(range((inner - 1).bit_length()))]:
        to = (flip(row, bit), col)
        started = exchange(
            [
                (i, number + n, raws[i].at[:, flip(seat, mask)], to)
                for n, mask in enumerate(held)
                for i in range(2)
            ]
        )
        number += len(held)
        held = held + [mask + bit for mask in held]
        if bit * 2 >= inner:
            advance(turned[: len(far_turned) // 2])
        else:
            advance(turned[len(far_turned) // 2 : len(far_turned)])
            advance((0, k) for k in near_all)
            ahead(len(straight))
        for copy in started:
            copy.wait_recv()
    advance(turned[len(far_turned) :])
    advance((part, k) for part in range(1, count) for k in near_all)

    per_point = span // NC
    fill(swap, lambda p, n: n == (p & (NC - 1)) * per_point + lax.div(p, NC), min(LANES, span))
    if fused:
        acc_ref[...] = jnp.zeros_like(acc_ref)

    for i, start in enumerate((0, lefts[0].shape[1])):
        raw, left = raws[i], lefts[i]
        bands = raw.shape[2]
        join = max(1, LANES // (inner * bands))
        width = join * inner * bands

        def scale(m, carry, raw=raw, left=left, start=start, width=width, join=join):
            lanes = pl.ds(pl.multiple_of(m * width, width), width)
            factors = decays[:, pl.ds(pl.multiple_of(start + m * width, LANES), width)]
            for t in range(window // LANES):
                piece = raw[pl.ds(m * join, join), :, :, pl.ds(t * LANES, LANES)]
                turned = piece.reshape(width, LANES).astype(jnp.float32).T * factors
                turned = turned.astype(jnp.bfloat16)
                for s in range(LANES // HALF_ROWS):
                    q = (t * LANES + s * HALF_ROWS) // (HALVES * HALF_ROWS)
                    at = ((s % HALVES) * row_count + q) * HALF_ROWS
                    left[pl.ds(at, HALF_ROWS), lanes] = turned[s * HALF_ROWS : (s + 1) * HALF_ROWS]
            return carry

        lax.fori_loop(0, outer // join, scale, 0)

    def product(h, turn, first, width):
        rows = pl.ds(h * block_rows, block_rows)
        lanes = pl.ds(turn * span + first, width)
        green = []
        for i in range(2):
            wave = planes[i][:, :, lanes]
            wave = wave.reshape(wave.shape[0] * wave.shape[1], width)
            green.append(dot(lefts[i][rows, :], wave))
        value = (green[0] * green[1] * factor).astype(jnp.bfloat16)
        return dot(value, swap[pl.ds(first, width), :])

    for copy in own[: 2 * turns]:
        copy.wait()
    ordered = [k for s in range(inner) for k in far if k % inner == s]
    quarter = len(ordered) // FARS
    fars = [ordered[n * quarter : (n + 1) * quarter] for n in range(FARS)]
    keep = []

    def to_row(h, ks, group):
        for k in ks:
            send(
                polar.at[h, peer(k)],
                x_ref.at[h, col, row],
                give_send.at[h],
                give_recv.at[h, group],
                (peer(k), col),
            ).start()

    def to_cols(h, ks):
        for k in ks:
            for d in range(1, col_count):
                slot = x_ref.at[h, col, row]
                if fused and h == turns * HALVES - 1:
                    slot = tail_x.at[d - 1, row]
                send(
                    polar.at[h, peer(k)],
                    slot,
                    pass_send.at[h],
                    pass_recv.at[h, d - 1, 0],
                    (peer(k), lax.rem(col + d, col_count)),
                ).start()

    def forward(h, group):
        some = fars[group]
        drain(x_ref.at[h, col, pl.ds(0, len(some))], give_recv.at[h, 1 + group])
        for k in some:
            arrived = x_ref.at[h, col, peer(k)]
            for d in range(1, col_count):
                slot = arrived
                if fused and h == turns * HALVES - 1:
                    slot = tail_x.at[d - 1, peer(k)]
                to = (row, lax.rem(col + d, col_count))
                send(arrived, slot, pass_send.at[h], pass_recv.at[h, d - 1, 1], to).start()

    def wait_near(h):
        drain(x_ref.at[h, col, pl.ds(0, near - 1)], give_recv.at[h, 0])
        keep[h].wait()

    def wait_pass(h, which):
        for d in range(1, col_count):
            count = row_count - near if which else near
            drain(x_ref.at[h, col, pl.ds(0, count)], pass_recv.at[h, d - 1, which])

    def give(h):
        copy = pltpu.make_async_copy(polar.at[h, row], x_ref.at[h, col, row], keep_sem.at[h])
        copy.start()
        keep.append(copy)
        to_cols(h, range(min(2, inner)))
        for group in range(FARS):
            to_row(h, fars[group], 1 + group)
        to_row(h, range(inner, near), 0)
        to_row(h, range(1, inner), 0)
        to_cols(h, range(min(2, inner), near))

    def form(part):
        wait_waves(part)
        turn, first, last = parts[part]
        tile = min(last - first, 2 * LANES)
        for h in range(HALVES):
            moved = mixed[h] if first else None
            for start in range(first, last, tile):
                term = product(h, turn, start, tile)
                moved = term if moved is None else moved + term
            if last < span:
                mixed[h] = moved
            else:
                g = turn * HALVES + h
                polar[g] = moved.astype(jnp.bfloat16).reshape(row_count, HALF_ROWS, span)
                give(g)

    if fused:
        for copy in own[2 * turns :]:
            copy.wait()
        wide = 2 * row_count * per_point
        middle = wide // 2
        tails = [
            pltpu.make_async_copy(line_ref, tail_line, tail_sem.at[0]),
        ]
        for d in range(1, col_count):
            c = lax.rem(col + col_count - d, col_count)
            depth = pl.multiple_of((c * turns + turns - 1) * wide, wide)
            for n, tail in enumerate((tail_cos, tail_sin)):
                part = plane_ref.at[pl.ds(depth + n * middle, middle)]
                tails.append(pltpu.make_async_copy(part, tail.at[d - 1], tail_sem.at[2 * d + n]))
        for copy in tails:
            copy.start()

        def transform(g, c):
            turn, h = divmod(g, HALVES)
            blocks = [x_ref.at[g, c, q] for q in range(row_count)]
            depth = pl.ds(pl.multiple_of((c * turns + turn) * wide, wide), wide)
            acc_ref[h] += dot(spread(blocks, lines_buf, line_ref), plane_ref[depth, :])

        def put_out(h):
            per_half = PIECES // HALVES
            height = acc_ref.shape[1] // (2 * per_half)
            for i in range(2):
                for n in range(per_half):
                    pltpu.make_async_copy(
                        acc_ref.at[h, pl.ds((i * per_half + n) * height, height)],
                        parts_out[i * PIECES + h * per_half + n],
                        out_sem.at[h],
                    ).start()

    else:

        def transform(g, c):
            return

        def put_out(h):
            return

        tails = []
    others = [lax.rem(col + d, col_count) for d in range(1, col_count)]

    def wait_passes(g):
        wait_pass(g, 0)
        wait_pass(g, 1)

    for part in range(len(parts)):
        form(part)
    last = turns * HALVES - 1
    pending = []

    def settle():
        g = pending.pop(0)
        wait_passes(g)
        for c in others:
            transform(g, c)
        if g + HALVES > last:
            put_out(g % HALVES)

    for g in range(last + 1):
        for group in range(FARS // 2):
            forward(g, group)
        if len(pending) > 1:
            settle()
        for group in range(FARS // 2, FARS):
            forward(g, group)
        wait_near(g)
        transform(g, col)
        pending.append(g)
    put_out(last % HALVES)
    while len(pending) > 1:
        settle()
    wait_passes(last)
    for copy in tails:
        copy.wait()
    if fused:
        for h in range(HALVES):
            drain(acc_ref.at[h], out_sem.at[h])

    for i in range(2):
        drain(planes[i].at[pl.ds(0, row_count - 1)], wave_send.at[i])
    for copy in sent:
        copy.wait_send()
    for h in range(turns * HALVES):
        drain(x_ref.at[h, col, pl.ds(0, row_count - 1)], give_send.at[h])
        for d in range(1, col_count):
            drain(x_ref.at[h, col], pass_send.at[h])

    @pl.when(col == 0)
    def _():
        for i in range(2):
            for c in range(1, col_count):
                over_col(i, c).wait_send()

    if not fused:
        for copy in own[2 * turns :]:
            copy.wait()


def whole(row_count, col_count, occ, vir, decays, window, factor):
    inner = group_size(row_count)
    outer = row_count // inner
    points = occ.shape[1] // row_count
    fused = points == NB * NC and row_count * col_count == NA and (row_count // 2) % (LANES // NB) == 0
    fused = fused and row_count % 2 == 0
    turns = 2 if fused else 1
    span = points // turns
    parts = tuple((turn, 0, span) for turn in range(turns))
    bands = (occ.shape[0], vir.shape[0])
    block_rows = row_count * HALF_ROWS
    bf16, f32 = jnp.bfloat16, jnp.float32
    dma = pltpu.SemaphoreType.DMA
    vmem = pl.BlockSpec(memory_space=pltpu.VMEM)
    hbm = pl.BlockSpec(memory_space=pltpu.HBM)
    x_shape = (turns * HALVES, col_count, row_count, HALF_ROWS, span)
    operands = [occ, vir, decays]
    in_specs = [hbm, hbm, vmem]
    scratch = [pltpu.VMEM((row_count, b, points), bf16) for b in bands]
    scratch += [pltpu.VMEM((outer, inner, b, window), bf16) for b in bands]
    scratch += [pltpu.VMEM((window, row_count * b), bf16) for b in bands]
    scratch += [
        pltpu.VMEM((HALVES, block_rows, span), f32),
        pltpu.VMEM((turns * HALVES, row_count, HALF_ROWS, span), bf16),
        pltpu.VMEM((span, span), bf16),
    ]
    if fused:
        cosine, sine = plane_tables(turns, row_count)
        depth = row_count * (span // NC)
        both = jnp.stack([cosine.reshape(-1, depth, NAB), sine.reshape(-1, depth, NAB)], axis=1)
        line = line_tables(col_count)
        flat = jnp.pad(line.reshape(-1, line.shape[2]), ((0, 0), (0, NAB - line.shape[2])))
        operands += [jnp.concatenate([both.reshape(-1, NAB), flat])]
        in_specs += [hbm]
        scratch += [
            pltpu.VMEM(x_shape, bf16),
            pltpu.VMEM(line.shape[1:], bf16),
            pltpu.VMEM((2 * NAB, NAB), bf16),
            pltpu.VMEM((NC * R_BLOCK, row_count * (span // NC)), bf16),
        ]
        scratch += [pltpu.VMEM((HALVES, line.shape[1], NAB), f32)]
        scratch += [dma((2,)), dma((HALVES,)), dma((2 * col_count,))]
        out_shape = [jax.ShapeDtypeStruct((HALVES * line.shape[1] // 2 // PIECES, NAB), f32)] * (2 * PIECES)
        late = col_count - 1
        tails = [(late, row_count, HALF_ROWS, span)] + [(late, depth, NAB)] * 2 + [line.shape[1:]]
        out_shape += [jax.ShapeDtypeStruct(shape, bf16) for shape in tails]
    else:
        out_shape = [jax.ShapeDtypeStruct(x_shape, bf16)]
    places = max(1, col_count - 1)
    steps = outer - 1 + inner - 1
    scratch += [dma((2,)), dma((2, len(parts))), dma((2, places)), dma((2,))]
    scratch += [dma((2, steps))] * 2 + [dma((2, places))] * 2
    gives = turns * HALVES
    scratch += [dma((gives,)), dma((gives, 1 + FARS)), dma((gives,)), dma((gives, places, 2))]
    scratch += [dma((turns, 2)), dma((2,)), dma((gives,))]
    cfg = (row_count, col_count, inner, turns, parts, factor, fused)
    result = pl.pallas_call(
        functools.partial(whole_kernel, cfg),
        out_shape=out_shape,
        in_specs=in_specs,
        out_specs=[pl.BlockSpec(memory_space=pl.ANY) if fused else vmem] * len(out_shape),
        scratch_shapes=scratch,
        compiler_params=pltpu.CompilerParams(
            collective_id=0, has_side_effects=True, vmem_limit_bytes=VMEM_LIMIT
        ),
    )(*operands)
    return fused, result


def last_kernel(*refs):
    parts = refs[: 2 * PIECES]
    tail_x, tail_cos, tail_sin, tail_line = refs[2 * PIECES : 2 * PIECES + 4]
    re_out, im_out, lines_buf, *acc, sems = refs[2 * PIECES + 4 :]
    outs = (re_out, im_out)
    half = PIECES // HALVES
    rows = parts[0].shape[0]
    copies = []

    def put(i, p, src):
        copy = pltpu.make_async_copy(src, outs[i].at[pl.ds(p * rows, rows)], sems.at[i, p])
        copy.start()
        copies.append(copy)

    for i in range(2):
        for p in range(half):
            put(i, p, parts[i * PIECES + p])
    late = []
    for d in range(tail_x.shape[0]):
        blocks = [tail_x.at[d, a] for a in range(tail_x.shape[1])]
        late.append((spread(blocks, lines_buf, tail_line), tail_cos[d], tail_sin[d]))
    for n in range(half):
        p = half + n
        for i in range(2):
            total = parts[i * PIECES + p][...]
            for both, cosine, sine in late:
                some = both[(i * half + n) * rows : (i * half + n + 1) * rows]
                middle = some.shape[1] // 2
                total = total + dot(some[:, :middle], cosine) + dot(some[:, middle:], sine)
            acc[i][pl.ds(n * rows, rows), :] = total
            put(i, p, acc[i].at[pl.ds(n * rows, rows)])
    for copy in copies:
        copy.wait()


def last(operands):
    rows, lanes = operands[0].shape
    vmem = pl.BlockSpec(memory_space=pltpu.VMEM)
    tail_x = operands[2 * PIECES]
    acc = pltpu.VMEM((rows * PIECES // HALVES, lanes), jnp.float32)
    return pl.pallas_call(
        last_kernel,
        out_shape=[jax.ShapeDtypeStruct((rows * PIECES, lanes), jnp.float32)] * 2,
        in_specs=[vmem] * len(operands),
        out_specs=[pl.BlockSpec(memory_space=pltpu.HBM)] * 2,
        scratch_shapes=[
            pltpu.VMEM((NC * R_BLOCK, operands[2 * PIECES + 1].shape[1]), jnp.bfloat16),
            acc,
            acc,
            pltpu.SemaphoreType.DMA((2, PIECES)),
        ],
        compiler_params=pltpu.CompilerParams(vmem_limit_bytes=8 * 1024 * 1024),
    )(*operands)


def on_device(rows_dev, occupied_waves, virtual_waves, occupied_decay, virtual_decay):
    row_count = lax.axis_size("row")
    col_count = lax.axis_size("col")
    nocc, nvir = occupied_decay.shape[0], virtual_decay.shape[0]
    window = rows_dev * row_count
    points = occupied_waves.shape[1] // row_count
    factor = -1.0 / math.sqrt(nocc * nvir) / math.sqrt(NGRID)
    fused, result = whole(
        row_count,
        col_count,
        occupied_waves,
        virtual_waves,
        jnp.concatenate([occupied_decay, virtual_decay]).reshape(1, nocc + nvir),
        window,
        factor,
    )
    if fused:
        real_part, imag_part = last(result)
    else:
        x = result[0].reshape(HALVES, col_count * row_count, R_BLOCK, NC, points // NC)
        x = jnp.transpose(x, (3, 0, 2, 1, 4)).reshape(NC, rows_dev, NAB)
        real_part, imag_part = spectrum(x, line_tables(col_count))
    shape = (rows_dev, NC // col_count, NAB)
    return real_part.reshape(shape), imag_part.reshape(shape)


ROWS_DEV = 32


def solution(mesh):
    in_specs = (P("row", "col"), P("row", "col"), P(), P())
    out_specs = (P("row", "col", None), P("row", "col", None))
    return jax.shard_map(
        functools.partial(on_device, ROWS_DEV),
        mesh=mesh,
        in_specs=in_specs,
        out_specs=out_specs,
        check_vma=False,
    )
```

```python
import functools
import math

import jax
import jax.numpy as jnp
import numpy as np
from jax import lax
from jax.experimental import pallas as pl
from jax.experimental.pallas import tpu as pltpu
from jax.sharding import PartitionSpec as P

NA = 32
NB = 32
NC = 32
NAB = NA * NB
NGRID = NA * NB * NC
LANES = 128
R_BLOCK = 16


def trig(phase, length):
    angle = (phase % length) * (2.0 * math.pi / length)
    return np.cos(angle), np.sin(angle)


def bf16_table(table):
    return jnp.asarray(table.astype(np.float32)).astype(jnp.bfloat16)


def plane_tables():
    index = np.arange(NAB)
    a, b = index // NB, index % NB
    phase = a[:, None] * a[None, :] * NB + b[:, None] * b[None, :] * NA
    cosine, sine = trig(phase, NA * NB)
    return bf16_table(cosine), bf16_table(sine)


def angle_tables():
    index = np.arange(NAB)
    first = trig(np.arange(NA)[:, None] * (index // NB)[None, :], NA)
    second = trig(np.arange(NB)[:, None] * (index % NB)[None, :], NB)
    return jnp.asarray(np.concatenate(first + second).astype(np.float32))


def line_tables(col_count):
    share = NC // col_count
    full = np.zeros((col_count, 2, R_BLOCK, share, NC, R_BLOCK))
    for y in range(col_count):
        kc = y * share + np.arange(share)
        cosine, sine = trig(kc[:, None] * np.arange(NC)[None, :], NC)
        for r in range(R_BLOCK):
            full[y, 0, r, :, :, r] = cosine
            full[y, 1, r, :, :, r] = -sine
    return bf16_table(full.reshape(col_count, 2 * R_BLOCK * share, NC * R_BLOCK))


def dot(a, b):
    return jnp.dot(a, b, preferred_element_type=jnp.float32)


def spectrum_kernel(x_ref, line_ref, cos_ref, sin_ref, re_ref, im_ref):
    rows = x_ref[...].reshape(NC * R_BLOCK, NAB)
    line = dot(line_ref[lax.axis_index("col")], rows).astype(jnp.bfloat16)
    half = line.shape[0] // 2
    re, im = line[:half], line[half:]
    re_ref[...] = dot(re, cos_ref[...]) + dot(im, sin_ref[...])
    im_ref[...] = dot(im, cos_ref[...]) - dot(re, sin_ref[...])


def spectrum(x, line_table):
    r_count = x.shape[1]
    cosine, sine = plane_tables()
    out_rows = line_table.shape[1] // 2
    steps = r_count // R_BLOCK
    whole = lambda table: pl.BlockSpec(table.shape, lambda i: (0,) * table.ndim)
    out = jax.ShapeDtypeStruct((out_rows * steps, NAB), jnp.float32)
    out_spec = pl.BlockSpec((out_rows, NAB), lambda i: (i, 0))
    return pl.pallas_call(
        spectrum_kernel,
        grid=(steps,),
        in_specs=[
            pl.BlockSpec((x.shape[0], R_BLOCK, x.shape[2]), lambda i: (0, i, 0)),
            whole(line_table),
            whole(cosine),
            whole(sine),
        ],
        out_specs=[out_spec, out_spec],
        out_shape=[out, out],
        compiler_params=pltpu.CompilerParams(vmem_limit_bytes=48 * 1024 * 1024),
    )(x, line_table, cosine, sine)


MESH = pl.DeviceIdType.MESH
HALVES = 2
VMEM_LIMIT = 48 * 1024 * 1024
PIECES = 4
FARS = 4
AHEAD = (1, 2, 1)
HALF_ROWS = R_BLOCK


def flip(index, mask):
    bits = [1 << bit for bit in range(mask.bit_length()) if mask >> bit & 1]
    for bit in bits:
        index = index + bit - 2 * bit * lax.rem(lax.div(index, bit), 2)
    return index


def group_size(row_count):
    return 4 if row_count % 4 == 0 else 1


def send(src, dst, send_sem, recv_sem, target):
    return pltpu.make_async_remote_copy(
        src_ref=src,
        dst_ref=dst,
        send_sem=send_sem,
        recv_sem=recv_sem,
        device_id=target,
        device_id_type=MESH,
    )


def drain(ref, sem):
    pltpu.make_async_copy(ref, ref, sem).wait()


def enter(row_count, col_count, inner, row, col):
    barrier = pltpu.get_barrier_semaphore()
    targets = [(flip(row, k), col) for k in range(1, row_count)]
    targets += [
        (flip(row, s), lax.rem(col + d, col_count))
        for d in range(1, col_count)
        for s in range(inner)
    ]
    for target in targets:
        pl.semaphore_signal(barrier, inc=1, device_id=target, device_id_type=MESH)
    return barrier, len(targets)


def fill(ref, values, rows):
    width = ref.shape[1]

    def step(i, carry):
        start = pl.multiple_of(i * rows, rows)
        row = lax.broadcasted_iota(jnp.int32, (rows, width), 0) + start
        lane = lax.broadcasted_iota(jnp.int32, (rows, width), 1)
        ref[pl.ds(start, rows), :] = jnp.where(values(row, lane), 1.0, 0.0).astype(jnp.bfloat16)
        return carry

    lax.fori_loop(0, ref.shape[0] // rows, step, 0)


def spread(blocks, lines_buf, line_table):
    short = blocks[0].shape[1] // NC
    per = LANES // short
    count = blocks[0].shape[1] // LANES
    groups = len(blocks) // per
    pieces = []
    for k in range(per):
        parts = [blocks[g * per + k][:, pl.ds(t * LANES, LANES)] for g in range(groups) for t in range(count)]
        pieces.append(jnp.concatenate(parts, axis=0))
    lane = lax.broadcasted_iota(jnp.int32, pieces[0].shape, 1)
    bit = per // 2
    while bit:
        high = (lane & (bit * short)) != 0
        for k in range(per):
            if k & bit:
                continue
            a, b = pieces[k], pieces[k + bit]
            pieces[k] = jnp.where(high, pltpu.roll(b, bit * short, 1), a)
            pieces[k + bit] = jnp.where(high, b, pltpu.roll(a, LANES - bit * short, 1))
        bit //= 2
    for g in range(groups):
        for t in range(count):
            at = (g * count + t) * R_BLOCK
            for j in range(per):
                place = pl.ds((t * per + j) * R_BLOCK, R_BLOCK)
                lines_buf[place, pl.ds(g * LANES, LANES)] = pieces[j][at : at + R_BLOCK]
    line = dot(line_table[...], lines_buf[...]).astype(jnp.bfloat16)
    half = line.shape[0] // 2
    re, im = line[:half], line[half:]
    return jnp.concatenate([jnp.concatenate([re, im], axis=1), jnp.concatenate([im, -re], axis=1)], axis=0)


def whole_kernel(cfg, *refs):
    (row_count, col_count, inner, turns, parts, factor, fused) = cfg
    refs = list(refs)
    take = lambda n: [refs.pop(0) for _ in range(n)]
    occ_ref, vir_ref, decays = take(3)
    if fused:
        line_hbm, angle_hbm = take(2)
        parts_out = take(2 * PIECES)
        tail_x, tail_cos, tail_sin, tail_line = take(4)
    else:
        (x_ref,) = take(1)
    planes = take(2)
    raws = take(2)
    lefts = take(2)
    mixed, polar, swap = take(3)
    if fused:
        x_ref, line_ref, angle_ref, plane_ref, lines_buf, acc_ref = take(6)
        table_sem, out_sem, tail_sem = take(3)
    (wave_send, wave_recv, col_send, col_recv, line_send, line_recv, share_send, share_recv) = take(8)
    (give_send, give_recv, pass_send, pass_recv, local, col_local, keep_sem) = take(7)

    row, col = lax.axis_index("row"), lax.axis_index("col")
    outer = row_count // inner
    mine, seat = lax.div(row, inner), lax.rem(row, inner)
    points = occ_ref.shape[1] // row_count
    waves = (occ_ref, vir_ref)
    window = raws[0].shape[3]
    share = window // col_count
    block_rows = row_count * HALF_ROWS

    def peer(k):
        return flip(row, k)

    barrier, arrivals = enter(row_count, col_count, inner, row, col)

    own = []
    span = points // turns

    def share_of(to, turn):
        return (lax.div(to, turns) * turns + turn) * points + lax.rem(to, turns) * span

    for turn in range(turns):
        for i in range(2):
            lanes = pl.ds(pl.multiple_of(share_of(row, turn), LANES), span)
            place = planes[i].at[row, :, pl.ds(turn * span, span)]
            own.append(pltpu.make_async_copy(waves[i].at[:, lanes], place, local.at[turn, i]))
    if fused:
        own.append(pltpu.make_async_copy(line_hbm.at[col], line_ref, table_sem.at[0]))
        own.append(pltpu.make_async_copy(angle_hbm, angle_ref, table_sem.at[1]))
    for copy in own:
        copy.start()
    pl.semaphore_wait(barrier, arrivals)

    def start_waves(part, ks):
        turn, first, last = parts[part]
        for k in ks:
            to = peer(k)
            lanes = pl.ds(pl.multiple_of(share_of(to, turn) + first, LANES), last - first)
            for i in range(2):
                copy = send(
                    waves[i].at[:, lanes],
                    planes[i].at[row, :, pl.ds(turn * span + first, last - first)],
                    wave_send.at[i],
                    wave_recv.at[i, part],
                    (to, col),
                )
                copy.start()

    def wait_waves(part):
        turn, first, last = parts[part]
        lanes = pl.ds(turn * span + first, last - first)
        for i in range(2):
            drain(planes[i].at[pl.ds(0, row_count - 1), :, lanes], wave_recv.at[i, part])

    near = row_count // 2

    def slab_share(c):
        return pl.ds(c * share, share) if isinstance(c, int) else pl.ds(pl.multiple_of(c * share, LANES), share)

    def over_col(i, c):
        return send(
            waves[i].at[:, slab_share(c)],
            raws[i].at[mine, seat, :, slab_share(c)],
            col_send.at[i, c - 1],
            col_recv.at[i],
            (row, c),
        )

    @pl.when(col == 0)
    def _():
        for i in range(2):
            for c in range(1, col_count):
                over_col(i, c).start()
            pltpu.make_async_copy(
                waves[i].at[:, slab_share(0)], raws[i].at[mine, seat, :, slab_share(0)], col_local.at[i]
            ).start()

    far = range(near, row_count)
    seats = [[k for k in far if k % inner == s] for s in range(inner)]
    count = len(parts)
    middle = inner // 2
    near_all = list(range(inner, near)) + list(range(1, inner))
    far_straight = [k for ks in seats[:middle] for k in ks]
    far_turned = [k for ks in seats[middle:] for k in ks]
    straight = [(part, k) for part in range(count) for k in far_straight]
    turned = [(part, k) for part in range(count) for k in far_turned]

    def advance(some):
        for part, k in some:
            start_waves(part, [k])

    def ahead(count):
        advance(straight[:count])
        del straight[:count]

    ahead(1)

    @pl.when(col == 0)
    def _():
        for i in range(2):
            pltpu.make_async_copy(
                waves[i].at[:, slab_share(0)], raws[i].at[mine, seat, :, slab_share(0)], col_local.at[i]
            ).wait()

    if col_count > 1:

        @pl.when(col != 0)
        def _():
            for i in range(2):
                over_col(i, 1).wait_recv()

    sent = []
    mine, seat = lax.div(row, inner), lax.rem(row, inner)

    def exchange(pairs):
        started = [send(place, place, line_send.at[i, n], line_recv.at[i, n], to) for i, n, place, to in pairs]
        for copy in started:
            copy.start()
        sent.extend(started)
        return started

    held = [0]
    number = 0
    for bit in [1 << bit for bit in reversed(range((outer - 1).bit_length()))]:
        to = (flip(row, bit * inner), col)
        started = exchange(
            [
                (i, number + n, raws[i].at[flip(mine, mask), seat, :, slab_share(col)], to)
                for n, mask in enumerate(held)
                for i in range(2)
            ]
        )
        number += len(held)
        held = held + [mask + bit for mask in held]
        ahead(AHEAD[0] if bit * 2 >= outer else AHEAD[1])
        for copy in started:
            copy.wait_recv()
    started = []
    for d in range(1, col_count):
        for i in range(2):
            place = raws[i].at[:, seat, :, slab_share(col)]
            to = (row, lax.rem(col + d, col_count))
            started.append(send(place, place, share_send.at[i, d - 1], share_recv.at[i, d - 1], to))
    for copy in started:
        copy.start()
    sent.extend(started)
    ahead(AHEAD[2])
    for copy in started:
        copy.wait_recv()
    held = [0]
    for bit in [1 << bit for bit in reversed(range((inner - 1).bit_length()))]:
        to = (flip(row, bit), col)
        started = exchange(
            [
                (i, number + n, raws[i].at[:, flip(seat, mask)], to)
                for n, mask in enumerate(held)
                for i in range(2)
            ]
        )
        number += len(held)
        held = held + [mask + bit for mask in held]
        if bit * 2 >= inner:
            advance(turned[: len(far_turned) // 2])
        else:
            advance(turned[len(far_turned) // 2 : len(far_turned)])
            advance((0, k) for k in near_all)
            ahead(len(straight))
        for copy in started:
            copy.wait_recv()
    advance(turned[len(far_turned) :])
    advance((part, k) for part in range(1, count) for k in near_all)

    per_point = span // NC
    fill(swap, lambda p, n: n == (p & (NC - 1)) * per_point + lax.div(p, NC), min(LANES, span))
    if fused:
        acc_ref[...] = jnp.zeros_like(acc_ref)
        for copy in own[2 * turns :]:
            copy.wait()
        depth = row_count * per_point

        def fill_planes(a, carry):
            within = lax.rem(a, row_count)
            turn = lax.div(a, row_count) * turns + lax.rem(within, turns)
            at = turn * 2 * depth + lax.div(within, turns) * NB
            cos_a, sin_a = angle_ref[pl.ds(a, 1), :], angle_ref[pl.ds(NA + a, 1), :]
            cos_b, sin_b = angle_ref[pl.ds(2 * NA, NB), :], angle_ref[pl.ds(2 * NA + NB, NB), :]
            cosine, sine = cos_a * cos_b - sin_a * sin_b, sin_a * cos_b + cos_a * sin_b
            plane_ref[pl.ds(pl.multiple_of(at, NB), NB), :] = cosine.astype(jnp.bfloat16)
            plane_ref[pl.ds(pl.multiple_of(at + depth, NB), NB), :] = sine.astype(jnp.bfloat16)
            return carry

        lax.fori_loop(0, NA, fill_planes, 0)

    for i, start in enumerate((0, lefts[0].shape[1])):
        raw, left = raws[i], lefts[i]
        bands = raw.shape[2]
        join = max(1, LANES // (inner * bands))
        width = join * inner * bands

        def scale(m, carry, raw=raw, left=left, start=start, width=width, join=join):
            lanes = pl.ds(pl.multiple_of(m * width, width), width)
            factors = decays[:, pl.ds(pl.multiple_of(start + m * width, LANES), width)]
            for t in range(window // LANES):
                piece = raw[pl.ds(m * join, join), :, :, pl.ds(t * LANES, LANES)]
                turned = piece.reshape(width, LANES).astype(jnp.float32).T * factors
                turned = turned.astype(jnp.bfloat16)
                for s in range(LANES // HALF_ROWS):
                    q = (t * LANES + s * HALF_ROWS) // (HALVES * HALF_ROWS)
                    at = ((s % HALVES) * row_count + q) * HALF_ROWS
                    left[pl.ds(at, HALF_ROWS), lanes] = turned[s * HALF_ROWS : (s + 1) * HALF_ROWS]
            return carry

        lax.fori_loop(0, outer // join, scale, 0)

    def product(h, turn, first, width):
        rows = pl.ds(h * block_rows, block_rows)
        lanes = pl.ds(turn * span + first, width)
        green = []
        for i in range(2):
            wave = planes[i][:, :, lanes]
            wave = wave.reshape(wave.shape[0] * wave.shape[1], width)
            green.append(dot(lefts[i][rows, :], wave))
        value = (green[0] * green[1] * factor).astype(jnp.bfloat16)
        return dot(value, swap[pl.ds(first, width), :])

    for copy in own[: 2 * turns]:
        copy.wait()
    ordered = [k for s in range(inner) for k in far if k % inner == s]
    quarter = len(ordered) // FARS
    fars = [ordered[n * quarter : (n + 1) * quarter] for n in range(FARS)]
    keep = []

    def to_row(h, ks, group):
        for k in ks:
            send(
                polar.at[h, peer(k)],
                x_ref.at[h, col, row],
                give_send.at[h],
                give_recv.at[h, group],
                (peer(k), col),
            ).start()

    def to_cols(h, ks):
        for k in ks:
            for d in range(1, col_count):
                slot = x_ref.at[h, col, row]
                if fused and h == turns * HALVES - 1:
                    slot = tail_x.at[d - 1, row]
                send(
                    polar.at[h, peer(k)],
                    slot,
                    pass_send.at[h],
                    pass_recv.at[h, d - 1, 0],
                    (peer(k), lax.rem(col + d, col_count)),
                ).start()

    def forward(h, group):
        some = fars[group]
        drain(x_ref.at[h, col, pl.ds(0, len(some))], give_recv.at[h, 1 + group])
        for k in some:
            arrived = x_ref.at[h, col, peer(k)]
            for d in range(1, col_count):
                slot = arrived
                if fused and h == turns * HALVES - 1:
                    slot = tail_x.at[d - 1, peer(k)]
                to = (row, lax.rem(col + d, col_count))
                send(arrived, slot, pass_send.at[h], pass_recv.at[h, d - 1, 1], to).start()

    def wait_near(h):
        drain(x_ref.at[h, col, pl.ds(0, near - 1)], give_recv.at[h, 0])
        keep[h].wait()

    def wait_pass(h, which):
        for d in range(1, col_count):
            count = row_count - near if which else near
            drain(x_ref.at[h, col, pl.ds(0, count)], pass_recv.at[h, d - 1, which])

    def give(h):
        copy = pltpu.make_async_copy(polar.at[h, row], x_ref.at[h, col, row], keep_sem.at[h])
        copy.start()
        keep.append(copy)
        to_cols(h, range(min(2, inner)))
        for group in range(FARS):
            to_row(h, fars[group], 1 + group)
        to_row(h, range(inner, near), 0)
        to_row(h, range(1, inner), 0)
        to_cols(h, range(min(2, inner), near))

    def form(part):
        wait_waves(part)
        turn, first, last = parts[part]
        tile = min(last - first, 2 * LANES)
        for h in range(HALVES):
            moved = mixed[h] if first else None
            for start in range(first, last, tile):
                term = product(h, turn, start, tile)
                moved = term if moved is None else moved + term
            if last < span:
                mixed[h] = moved
            else:
                g = turn * HALVES + h
                polar[g] = moved.astype(jnp.bfloat16).reshape(row_count, HALF_ROWS, span)
                give(g)

    if fused:
        wide = 2 * row_count * per_point
        middle = wide // 2
        tails = [
            pltpu.make_async_copy(line_ref, tail_line, tail_sem.at[0]),
        ]
        for d in range(1, col_count):
            c = lax.rem(col + col_count - d, col_count)
            depth = pl.multiple_of((c * turns + turns - 1) * wide, wide)
            for n, tail in enumerate((tail_cos, tail_sin)):
                part = plane_ref.at[pl.ds(depth + n * middle, middle)]
                tails.append(pltpu.make_async_copy(part, tail.at[d - 1], tail_sem.at[2 * d + n]))
        for copy in tails:
            copy.start()

        def transform(g, c):
            turn, h = divmod(g, HALVES)
            blocks = [x_ref.at[g, c, q] for q in range(row_count)]
            depth = pl.ds(pl.multiple_of((c * turns + turn) * wide, wide), wide)
            acc_ref[h] += dot(spread(blocks, lines_buf, line_ref), plane_ref[depth, :])

        def put_out(h):
            per_half = PIECES // HALVES
            height = acc_ref.shape[1] // (2 * per_half)
            for i in range(2):
                for n in range(per_half):
                    pltpu.make_async_copy(
                        acc_ref.at[h, pl.ds((i * per_half + n) * height, height)],
                        parts_out[i * PIECES + h * per_half + n],
                        out_sem.at[h],
                    ).start()

    else:

        def transform(g, c):
            return

        def put_out(h):
            return

        tails = []
    others = [lax.rem(col + d, col_count) for d in range(1, col_count)]

    def wait_passes(g):
        wait_pass(g, 0)
        wait_pass(g, 1)

    for part in range(len(parts)):
        form(part)
    last = turns * HALVES - 1
    pending = []

    def settle():
        g = pending.pop(0)
        wait_passes(g)
        for c in others:
            transform(g, c)
        if g + HALVES > last:
            put_out(g % HALVES)

    for g in range(last + 1):
        for group in range(FARS // 2):
            forward(g, group)
        if len(pending) > 1:
            settle()
        for group in range(FARS // 2, FARS):
            forward(g, group)
        wait_near(g)
        transform(g, col)
        pending.append(g)
    put_out(last % HALVES)
    while len(pending) > 1:
        settle()
    wait_passes(last)
    for copy in tails:
        copy.wait()
    if fused:
        for h in range(HALVES):
            drain(acc_ref.at[h], out_sem.at[h])

    for i in range(2):
        drain(planes[i].at[pl.ds(0, row_count - 1)], wave_send.at[i])
    for copy in sent:
        copy.wait_send()
    for h in range(turns * HALVES):
        drain(x_ref.at[h, col, pl.ds(0, row_count - 1)], give_send.at[h])
        for d in range(1, col_count):
            drain(x_ref.at[h, col], pass_send.at[h])

    @pl.when(col == 0)
    def _():
        for i in range(2):
            for c in range(1, col_count):
                over_col(i, c).wait_send()

    if not fused:
        for copy in own[2 * turns :]:
            copy.wait()


def whole(row_count, col_count, occ, vir, decays, window, factor):
    inner = group_size(row_count)
    outer = row_count // inner
    points = occ.shape[1] // row_count
    fused = points == NB * NC and row_count * col_count == NA and (row_count // 2) % (LANES // NB) == 0
    fused = fused and row_count % 2 == 0
    turns = 2 if fused else 1
    span = points // turns
    parts = tuple((turn, 0, span) for turn in range(turns))
    bands = (occ.shape[0], vir.shape[0])
    block_rows = row_count * HALF_ROWS
    bf16, f32 = jnp.bfloat16, jnp.float32
    dma = pltpu.SemaphoreType.DMA
    vmem = pl.BlockSpec(memory_space=pltpu.VMEM)
    hbm = pl.BlockSpec(memory_space=pltpu.HBM)
    x_shape = (turns * HALVES, col_count, row_count, HALF_ROWS, span)
    operands = [occ, vir, decays]
    in_specs = [hbm, hbm, vmem]
    scratch = [pltpu.VMEM((row_count, b, points), bf16) for b in bands]
    scratch += [pltpu.VMEM((outer, inner, b, window), bf16) for b in bands]
    scratch += [pltpu.VMEM((window, row_count * b), bf16) for b in bands]
    scratch += [
        pltpu.VMEM((HALVES, block_rows, span), f32),
        pltpu.VMEM((turns * HALVES, row_count, HALF_ROWS, span), bf16),
        pltpu.VMEM((span, span), bf16),
    ]
    if fused:
        line, angles = line_tables(col_count), angle_tables()
        depth = row_count * (span // NC)
        operands += [line, angles]
        in_specs += [hbm] * 2
        scratch += [
            pltpu.VMEM(x_shape, bf16),
            pltpu.VMEM(line.shape[1:], bf16),
            pltpu.VMEM(angles.shape, f32),
            pltpu.VMEM((2 * NAB, NAB), bf16),
            pltpu.VMEM((NC * R_BLOCK, row_count * (span // NC)), bf16),
        ]
        scratch += [pltpu.VMEM((HALVES, line.shape[1], NAB), f32)]
        scratch += [dma((2,)), dma((HALVES,)), dma((2 * col_count,))]
        out_shape = [jax.ShapeDtypeStruct((HALVES * line.shape[1] // 2 // PIECES, NAB), f32)] * (2 * PIECES)
        late = col_count - 1
        tails = [(late, row_count, HALF_ROWS, span)] + [(late, depth, NAB)] * 2 + [line.shape[1:]]
        out_shape += [jax.ShapeDtypeStruct(shape, bf16) for shape in tails]
    else:
        out_shape = [jax.ShapeDtypeStruct(x_shape, bf16)]
    places = max(1, col_count - 1)
    steps = outer - 1 + inner - 1
    scratch += [dma((2,)), dma((2, len(parts))), dma((2, places)), dma((2,))]
    scratch += [dma((2, steps))] * 2 + [dma((2, places))] * 2
    gives = turns * HALVES
    scratch += [dma((gives,)), dma((gives, 1 + FARS)), dma((gives,)), dma((gives, places, 2))]
    scratch += [dma((turns, 2)), dma((2,)), dma((gives,))]
    cfg = (row_count, col_count, inner, turns, parts, factor, fused)
    result = pl.pallas_call(
        functools.partial(whole_kernel, cfg),
        out_shape=out_shape,
        in_specs=in_specs,
        out_specs=[pl.BlockSpec(memory_space=pl.ANY) if fused else vmem] * len(out_shape),
        scratch_shapes=scratch,
        compiler_params=pltpu.CompilerParams(
            collective_id=0, has_side_effects=True, vmem_limit_bytes=VMEM_LIMIT
        ),
    )(*operands)
    return fused, result


def last_kernel(*refs):
    parts = refs[: 2 * PIECES]
    tail_x, tail_cos, tail_sin, tail_line = refs[2 * PIECES : 2 * PIECES + 4]
    re_out, im_out, lines_buf, *acc, sems = refs[2 * PIECES + 4 :]
    outs = (re_out, im_out)
    half = PIECES // HALVES
    rows = parts[0].shape[0]
    copies = []

    def put(i, p, src):
        copy = pltpu.make_async_copy(src, outs[i].at[pl.ds(p * rows, rows)], sems.at[i, p])
        copy.start()
        copies.append(copy)

    for i in range(2):
        for p in range(half):
            put(i, p, parts[i * PIECES + p])
    late = []
    for d in range(tail_x.shape[0]):
        blocks = [tail_x.at[d, a] for a in range(tail_x.shape[1])]
        late.append((spread(blocks, lines_buf, tail_line), tail_cos[d], tail_sin[d]))
    for n in range(half):
        p = half + n
        for i in range(2):
            total = parts[i * PIECES + p][...]
            for both, cosine, sine in late:
                some = both[(i * half + n) * rows : (i * half + n + 1) * rows]
                middle = some.shape[1] // 2
                total = total + dot(some[:, :middle], cosine) + dot(some[:, middle:], sine)
            acc[i][pl.ds(n * rows, rows), :] = total
            put(i, p, acc[i].at[pl.ds(n * rows, rows)])
    for copy in copies:
        copy.wait()


def last(operands):
    rows, lanes = operands[0].shape
    vmem = pl.BlockSpec(memory_space=pltpu.VMEM)
    tail_x = operands[2 * PIECES]
    acc = pltpu.VMEM((rows * PIECES // HALVES, lanes), jnp.float32)
    return pl.pallas_call(
        last_kernel,
        out_shape=[jax.ShapeDtypeStruct((rows * PIECES, lanes), jnp.float32)] * 2,
        in_specs=[vmem] * len(operands),
        out_specs=[pl.BlockSpec(memory_space=pltpu.HBM)] * 2,
        scratch_shapes=[
            pltpu.VMEM((NC * R_BLOCK, operands[2 * PIECES + 1].shape[1]), jnp.bfloat16),
            acc,
            acc,
            pltpu.SemaphoreType.DMA((2, PIECES)),
        ],
        compiler_params=pltpu.CompilerParams(vmem_limit_bytes=8 * 1024 * 1024),
    )(*operands)


def on_device(rows_dev, occupied_waves, virtual_waves, occupied_decay, virtual_decay):
    row_count = lax.axis_size("row")
    col_count = lax.axis_size("col")
    nocc, nvir = occupied_decay.shape[0], virtual_decay.shape[0]
    window = rows_dev * row_count
    points = occupied_waves.shape[1] // row_count
    factor = -1.0 / math.sqrt(nocc * nvir) / math.sqrt(NGRID)
    fused, result = whole(
        row_count,
        col_count,
        occupied_waves,
        virtual_waves,
        jnp.concatenate([occupied_decay, virtual_decay]).reshape(1, nocc + nvir),
        window,
        factor,
    )
    if fused:
        real_part, imag_part = last(result)
    else:
        x = result[0].reshape(HALVES, col_count * row_count, R_BLOCK, NC, points // NC)
        x = jnp.transpose(x, (3, 0, 2, 1, 4)).reshape(NC, rows_dev, NAB)
        real_part, imag_part = spectrum(x, line_tables(col_count))
    shape = (rows_dev, NC // col_count, NAB)
    return real_part.reshape(shape), imag_part.reshape(shape)


ROWS_DEV = 32


def solution(mesh):
    in_specs = (P("row", "col"), P("row", "col"), P(), P())
    out_specs = (P("row", "col", None), P("row", "col", None))
    return jax.shard_map(
        functools.partial(on_device, ROWS_DEV),
        mesh=mesh,
        in_specs=in_specs,
        out_specs=out_specs,
        check_vma=False,
    )
```

```python
import functools
import math

import jax
import jax.numpy as jnp
import numpy as np
from jax import lax
from jax.experimental import pallas as pl
from jax.experimental.pallas import tpu as pltpu
from jax.sharding import PartitionSpec as P

NA = 32
NB = 32
NC = 32
NAB = NA * NB
NGRID = NA * NB * NC
LANES = 128
R_BLOCK = 16


def trig(phase, length):
    angle = (phase % length) * (2.0 * math.pi / length)
    return np.cos(angle), np.sin(angle)


def bf16_table(table):
    return jnp.asarray(table.astype(np.float32)).astype(jnp.bfloat16)


def plane_tables():
    index = np.arange(NAB)
    a, b = index // NB, index % NB
    phase = a[:, None] * a[None, :] * NB + b[:, None] * b[None, :] * NA
    cosine, sine = trig(phase, NA * NB)
    return bf16_table(cosine), bf16_table(sine)


def angle_tables():
    index = np.arange(NAB)
    first = trig(np.arange(NA)[:, None] * (index // NB)[None, :], NA)
    second = trig(np.arange(NB)[:, None] * (index % NB)[None, :], NB)
    return jnp.asarray(np.concatenate(first + second).astype(np.float32))


def line_tables(col_count):
    share = NC // col_count
    full = np.zeros((col_count, 2, R_BLOCK, share, NC, R_BLOCK))
    for y in range(col_count):
        kc = y * share + np.arange(share)
        cosine, sine = trig(kc[:, None] * np.arange(NC)[None, :], NC)
        for r in range(R_BLOCK):
            full[y, 0, r, :, :, r] = cosine
            full[y, 1, r, :, :, r] = -sine
    return bf16_table(full.reshape(col_count, 2 * R_BLOCK * share, NC * R_BLOCK))


def dot(a, b):
    return jnp.dot(a, b, preferred_element_type=jnp.float32)


def spectrum_kernel(x_ref, line_ref, cos_ref, sin_ref, re_ref, im_ref):
    rows = x_ref[...].reshape(NC * R_BLOCK, NAB)
    line = dot(line_ref[lax.axis_index("col")], rows).astype(jnp.bfloat16)
    half = line.shape[0] // 2
    re, im = line[:half], line[half:]
    re_ref[...] = dot(re, cos_ref[...]) + dot(im, sin_ref[...])
    im_ref[...] = dot(im, cos_ref[...]) - dot(re, sin_ref[...])


def spectrum(x, line_table):
    r_count = x.shape[1]
    cosine, sine = plane_tables()
    out_rows = line_table.shape[1] // 2
    steps = r_count // R_BLOCK
    whole = lambda table: pl.BlockSpec(table.shape, lambda i: (0,) * table.ndim)
    out = jax.ShapeDtypeStruct((out_rows * steps, NAB), jnp.float32)
    out_spec = pl.BlockSpec((out_rows, NAB), lambda i: (i, 0))
    return pl.pallas_call(
        spectrum_kernel,
        grid=(steps,),
        in_specs=[
            pl.BlockSpec((x.shape[0], R_BLOCK, x.shape[2]), lambda i: (0, i, 0)),
            whole(line_table),
            whole(cosine),
            whole(sine),
        ],
        out_specs=[out_spec, out_spec],
        out_shape=[out, out],
        compiler_params=pltpu.CompilerParams(vmem_limit_bytes=48 * 1024 * 1024),
    )(x, line_table, cosine, sine)


MESH = pl.DeviceIdType.MESH
HALVES = 2
VMEM_LIMIT = 48 * 1024 * 1024
PIECES = 4
FARS = 4
AHEAD = (1, 2, 1)
HALF_ROWS = R_BLOCK


def flip(index, mask):
    bits = [1 << bit for bit in range(mask.bit_length()) if mask >> bit & 1]
    for bit in bits:
        index = index + bit - 2 * bit * lax.rem(lax.div(index, bit), 2)
    return index


def group_size(row_count):
    return 4 if row_count % 4 == 0 else 1


def send(src, dst, send_sem, recv_sem, target):
    return pltpu.make_async_remote_copy(
        src_ref=src,
        dst_ref=dst,
        send_sem=send_sem,
        recv_sem=recv_sem,
        device_id=target,
        device_id_type=MESH,
    )


def drain(ref, sem):
    pltpu.make_async_copy(ref, ref, sem).wait()


def enter(row_count, col_count, inner, row, col):
    barrier = pltpu.get_barrier_semaphore()
    targets = [(flip(row, k), col) for k in range(1, row_count)]
    targets += [
        (flip(row, s), lax.rem(col + d, col_count))
        for d in range(1, col_count)
        for s in range(inner)
    ]
    for target in targets:
        pl.semaphore_signal(barrier, inc=1, device_id=target, device_id_type=MESH)
    return barrier, len(targets)


def fill(ref, values, rows):
    width = ref.shape[1]

    def step(i, carry):
        start = pl.multiple_of(i * rows, rows)
        row = lax.broadcasted_iota(jnp.int32, (rows, width), 0) + start
        lane = lax.broadcasted_iota(jnp.int32, (rows, width), 1)
        ref[pl.ds(start, rows), :] = jnp.where(values(row, lane), 1.0, 0.0).astype(jnp.bfloat16)
        return carry

    lax.fori_loop(0, ref.shape[0] // rows, step, 0)


def spread(blocks, lines_buf, line_table):
    short = blocks[0].shape[1] // NC
    per = LANES // short
    count = blocks[0].shape[1] // LANES
    groups = len(blocks) // per
    pieces = []
    for k in range(per):
        parts = [blocks[g * per + k][:, pl.ds(t * LANES, LANES)] for g in range(groups) for t in range(count)]
        pieces.append(jnp.concatenate(parts, axis=0))
    lane = lax.broadcasted_iota(jnp.int32, pieces[0].shape, 1)
    bit = per // 2
    while bit:
        high = (lane & (bit * short)) != 0
        for k in range(per):
            if k & bit:
                continue
            a, b = pieces[k], pieces[k + bit]
            pieces[k] = jnp.where(high, pltpu.roll(b, bit * short, 1), a)
            pieces[k + bit] = jnp.where(high, b, pltpu.roll(a, LANES - bit * short, 1))
        bit //= 2
    for g in range(groups):
        for t in range(count):
            at = (g * count + t) * R_BLOCK
            for j in range(per):
                place = pl.ds((t * per + j) * R_BLOCK, R_BLOCK)
                lines_buf[place, pl.ds(g * LANES, LANES)] = pieces[j][at : at + R_BLOCK]
    line = dot(line_table[...], lines_buf[...]).astype(jnp.bfloat16)
    half = line.shape[0] // 2
    re, im = line[:half], line[half:]
    return jnp.concatenate([jnp.concatenate([re, im], axis=1), jnp.concatenate([im, -re], axis=1)], axis=0)


def whole_kernel(cfg, *refs):
    (row_count, col_count, inner, turns, parts, factor, fused) = cfg
    refs = list(refs)
    take = lambda n: [refs.pop(0) for _ in range(n)]
    occ_ref, vir_ref, decays = take(3)
    if fused:
        line_hbm, angle_hbm = take(2)
        parts_out = take(2 * PIECES)
        tail_x, tail_cos, tail_sin, tail_line = take(4)
    else:
        (x_ref,) = take(1)
    planes = take(2)
    raws = take(2)
    lefts = take(2)
    mixed, polar, swap = take(3)
    if fused:
        x_ref, line_ref, angle_ref, plane_ref, lines_buf, acc_ref = take(6)
        table_sem, out_sem, tail_sem = take(3)
    (wave_send, wave_recv, col_send, col_recv, line_send, line_recv, share_send, share_recv) = take(8)
    (give_send, give_recv, pass_send, pass_recv, local, col_local, keep_sem) = take(7)

    row, col = lax.axis_index("row"), lax.axis_index("col")
    outer = row_count // inner
    mine, seat = lax.div(row, inner), lax.rem(row, inner)
    points = occ_ref.shape[1] // row_count
    waves = (occ_ref, vir_ref)
    window = raws[0].shape[3]
    share = window // col_count
    block_rows = row_count * HALF_ROWS

    def peer(k):
        return flip(row, k)

    barrier, arrivals = enter(row_count, col_count, inner, row, col)

    own = []
    span = points // turns

    def share_of(to, turn):
        return (lax.div(to, turns) * turns + turn) * points + lax.rem(to, turns) * span

    for turn in range(turns):
        for i in range(2):
            lanes = pl.ds(pl.multiple_of(share_of(row, turn), LANES), span)
            place = planes[i].at[row, :, pl.ds(turn * span, span)]
            own.append(pltpu.make_async_copy(waves[i].at[:, lanes], place, local.at[turn, i]))
    if fused:
        own.append(pltpu.make_async_copy(line_hbm.at[col], line_ref, table_sem.at[0]))
        own.append(pltpu.make_async_copy(angle_hbm, angle_ref, table_sem.at[1]))
    for copy in own:
        copy.start()
    pl.semaphore_wait(barrier, arrivals)

    def start_waves(part, ks):
        turn, first, last = parts[part]
        for k in ks:
            to = peer(k)
            lanes = pl.ds(pl.multiple_of(share_of(to, turn) + first, LANES), last - first)
            for i in range(2):
                copy = send(
                    waves[i].at[:, lanes],
                    planes[i].at[row, :, pl.ds(turn * span + first, last - first)],
                    wave_send.at[i],
                    wave_recv.at[i, part],
                    (to, col),
                )
                copy.start()

    def wait_waves(part):
        turn, first, last = parts[part]
        lanes = pl.ds(turn * span + first, last - first)
        for i in range(2):
            drain(planes[i].at[pl.ds(0, row_count - 1), :, lanes], wave_recv.at[i, part])

    near = row_count // 2

    def slab_share(c):
        return pl.ds(c * share, share) if isinstance(c, int) else pl.ds(pl.multiple_of(c * share, LANES), share)

    def over_col(i, c):
        return send(
            waves[i].at[:, slab_share(c)],
            raws[i].at[mine, seat, :, slab_share(c)],
            col_send.at[i, c - 1],
            col_recv.at[i],
            (row, c),
        )

    @pl.when(col == 0)
    def _():
        for i in range(2):
            for c in range(1, col_count):
                over_col(i, c).start()
            pltpu.make_async_copy(
                waves[i].at[:, slab_share(0)], raws[i].at[mine, seat, :, slab_share(0)], col_local.at[i]
            ).start()

    far = range(near, row_count)
    seats = [[k for k in far if k % inner == s] for s in range(inner)]
    count = len(parts)
    middle = inner // 2
    near_all = list(range(inner, near)) + list(range(1, inner))
    far_straight = [k for ks in seats[:middle] for k in ks]
    far_turned = [k for ks in seats[middle:] for k in ks]
    straight = [(part, k) for part in range(count) for k in far_straight]
    turned = [(part, k) for part in range(count) for k in far_turned]

    def advance(some):
        for part, k in some:
            start_waves(part, [k])

    def ahead(count):
        advance(straight[:count])
        del straight[:count]

    ahead(1)

    @pl.when(col == 0)
    def _():
        for i in range(2):
            pltpu.make_async_copy(
                waves[i].at[:, slab_share(0)], raws[i].at[mine, seat, :, slab_share(0)], col_local.at[i]
            ).wait()

    if col_count > 1:

        @pl.when(col != 0)
        def _():
            for i in range(2):
                over_col(i, 1).wait_recv()

    sent = []
    mine, seat = lax.div(row, inner), lax.rem(row, inner)

    def exchange(pairs):
        started = [send(place, place, line_send.at[i, n], line_recv.at[i, n], to) for i, n, place, to in pairs]
        for copy in started:
            copy.start()
        sent.extend(started)
        return started

    held = [0]
    number = 0
    for bit in [1 << bit for bit in reversed(range((outer - 1).bit_length()))]:
        to = (flip(row, bit * inner), col)
        started = exchange(
            [
                (i, number + n, raws[i].at[flip(mine, mask), seat, :, slab_share(col)], to)
                for n, mask in enumerate(held)
                for i in range(2)
            ]
        )
        number += len(held)
        held = held + [mask + bit for mask in held]
        ahead(AHEAD[0] if bit * 2 >= outer else AHEAD[1])
        for copy in started:
            copy.wait_recv()
    started = []
    for d in range(1, col_count):
        for i in range(2):
            place = raws[i].at[:, seat, :, slab_share(col)]
            to = (row, lax.rem(col + d, col_count))
            started.append(send(place, place, share_send.at[i, d - 1], share_recv.at[i, d - 1], to))
    for copy in started:
        copy.start()
    sent.extend(started)
    ahead(AHEAD[2])
    for copy in started:
        copy.wait_recv()
    held = [0]
    for bit in [1 << bit for bit in reversed(range((inner - 1).bit_length()))]:
        to = (flip(row, bit), col)
        started = exchange(
            [
                (i, number + n, raws[i].at[:, flip(seat, mask)], to)
                for n, mask in enumerate(held)
                for i in range(2)
            ]
        )
        number += len(held)
        held = held + [mask + bit for mask in held]
        if bit * 2 >= inner:
            advance(turned[: len(far_turned) // 2])
        else:
            advance(turned[len(far_turned) // 2 : len(far_turned)])
            advance((0, k) for k in near_all)
            ahead(len(straight))
        for copy in started:
            copy.wait_recv()
    advance(turned[len(far_turned) :])
    advance((part, k) for part in range(1, count) for k in near_all)

    per_point = span // NC
    fill(swap, lambda p, n: n == (p & (NC - 1)) * per_point + lax.div(p, NC), min(LANES, span))
    if fused:
        acc_ref[...] = jnp.zeros_like(acc_ref)
        for copy in own[2 * turns :]:
            copy.wait()
        depth = row_count * per_point

        def fill_planes(a, carry):
            within = lax.rem(a, row_count)
            turn = lax.div(a, row_count) * turns + lax.rem(within, turns)
            at = turn * 2 * depth + lax.div(within, turns) * NB
            cos_a, sin_a = angle_ref[pl.ds(a, 1), :], angle_ref[pl.ds(NA + a, 1), :]
            cos_b, sin_b = angle_ref[pl.ds(2 * NA, NB), :], angle_ref[pl.ds(2 * NA + NB, NB), :]
            cosine, sine = cos_a * cos_b - sin_a * sin_b, sin_a * cos_b + cos_a * sin_b
            plane_ref[pl.ds(pl.multiple_of(at, NB), NB), :] = cosine.astype(jnp.bfloat16)
            plane_ref[pl.ds(pl.multiple_of(at + depth, NB), NB), :] = sine.astype(jnp.bfloat16)
            return carry

        lax.fori_loop(0, NA, fill_planes, 0)

    for i, start in enumerate((0, lefts[0].shape[1])):
        raw, left = raws[i], lefts[i]
        bands = raw.shape[2]
        join = max(1, LANES // (inner * bands))
        width = join * inner * bands

        def scale(m, carry, raw=raw, left=left, start=start, width=width, join=join):
            lanes = pl.ds(pl.multiple_of(m * width, width), width)
            factors = decays[:, pl.ds(pl.multiple_of(start + m * width, LANES), width)]
            for t in range(window // LANES):
                piece = raw[pl.ds(m * join, join), :, :, pl.ds(t * LANES, LANES)]
                turned = piece.reshape(width, LANES).astype(jnp.float32).T * factors
                turned = turned.astype(jnp.bfloat16)
                for s in range(LANES // HALF_ROWS):
                    q = (t * LANES + s * HALF_ROWS) // (HALVES * HALF_ROWS)
                    at = ((s % HALVES) * row_count + q) * HALF_ROWS
                    left[pl.ds(at, HALF_ROWS), lanes] = turned[s * HALF_ROWS : (s + 1) * HALF_ROWS]
            return carry

        lax.fori_loop(0, outer // join, scale, 0)

    def product(h, turn, first, width):
        rows = pl.ds(h * block_rows, block_rows)
        lanes = pl.ds(turn * span + first, width)
        green = []
        for i in range(2):
            wave = planes[i][:, :, lanes]
            wave = wave.reshape(wave.shape[0] * wave.shape[1], width)
            green.append(dot(lefts[i][rows, :], wave))
        value = (green[0] * green[1] * factor).astype(jnp.bfloat16)
        return dot(value, swap[pl.ds(first, width), :])

    for copy in own[: 2 * turns]:
        copy.wait()
    ordered = [k for s in range(inner) for k in far if k % inner == s]
    quarter = len(ordered) // FARS
    fars = [ordered[n * quarter : (n + 1) * quarter] for n in range(FARS)]
    keep = []

    def to_row(h, ks, group):
        for k in ks:
            send(
                polar.at[h, peer(k)],
                x_ref.at[h, col, row],
                give_send.at[0],
                give_recv.at[h, group],
                (peer(k), col),
            ).start()

    def to_cols(h, ks):
        for k in ks:
            for d in range(1, col_count):
                slot = x_ref.at[h, col, row]
                if fused and h == turns * HALVES - 1:
                    slot = tail_x.at[d - 1, row]
                send(
                    polar.at[h, peer(k)],
                    slot,
                    pass_send.at[0],
                    pass_recv.at[h, d - 1, 0],
                    (peer(k), lax.rem(col + d, col_count)),
                ).start()

    def forward(h, group):
        some = fars[group]
        drain(x_ref.at[h, col, pl.ds(0, len(some))], give_recv.at[h, 1 + group])
        for k in some:
            arrived = x_ref.at[h, col, peer(k)]
            for d in range(1, col_count):
                slot = arrived
                if fused and h == turns * HALVES - 1:
                    slot = tail_x.at[d - 1, peer(k)]
                to = (row, lax.rem(col + d, col_count))
                send(arrived, slot, pass_send.at[0], pass_recv.at[h, d - 1, 1], to).start()

    def wait_near(h):
        drain(x_ref.at[h, col, pl.ds(0, near - 1)], give_recv.at[h, 0])
        keep[h].wait()

    def wait_pass(h, which):
        for d in range(1, col_count):
            count = row_count - near if which else near
            drain(x_ref.at[h, col, pl.ds(0, count)], pass_recv.at[h, d - 1, which])

    def give(h):
        copy = pltpu.make_async_copy(polar.at[h, row], x_ref.at[h, col, row], keep_sem.at[h])
        copy.start()
        keep.append(copy)
        to_cols(h, range(min(2, inner)))
        for group in range(FARS):
            to_row(h, fars[group], 1 + group)
        to_row(h, range(inner, near), 0)
        to_row(h, range(1, inner), 0)
        to_cols(h, range(min(2, inner), near))

    def form(part):
        wait_waves(part)
        turn, first, last = parts[part]
        tile = min(last - first, 2 * LANES)
        for h in range(HALVES):
            moved = mixed[h] if first else None
            for start in range(first, last, tile):
                term = product(h, turn, start, tile)
                moved = term if moved is None else moved + term
            if last < span:
                mixed[h] = moved
            else:
                g = turn * HALVES + h
                polar[g] = moved.astype(jnp.bfloat16).reshape(row_count, HALF_ROWS, span)
                give(g)

    if fused:
        wide = 2 * row_count * per_point
        middle = wide // 2
        tails = [
            pltpu.make_async_copy(line_ref, tail_line, tail_sem.at[0]),
        ]
        for d in range(1, col_count):
            c = lax.rem(col + col_count - d, col_count)
            depth = pl.multiple_of((c * turns + turns - 1) * wide, wide)
            for n, tail in enumerate((tail_cos, tail_sin)):
                part = plane_ref.at[pl.ds(depth + n * middle, middle)]
                tails.append(pltpu.make_async_copy(part, tail.at[d - 1], tail_sem.at[2 * d + n]))
        for copy in tails:
            copy.start()

        def transform(g, c):
            turn, h = divmod(g, HALVES)
            blocks = [x_ref.at[g, c, q] for q in range(row_count)]
            depth = pl.ds(pl.multiple_of((c * turns + turn) * wide, wide), wide)
            acc_ref[h] += dot(spread(blocks, lines_buf, line_ref), plane_ref[depth, :])

        def put_out(h):
            per_half = PIECES // HALVES
            height = acc_ref.shape[1] // (2 * per_half)
            for i in range(2):
                for n in range(per_half):
                    pltpu.make_async_copy(
                        acc_ref.at[h, pl.ds((i * per_half + n) * height, height)],
                        parts_out[i * PIECES + h * per_half + n],
                        out_sem.at[h],
                    ).start()

    else:

        def transform(g, c):
            return

        def put_out(h):
            return

        tails = []
    others = [lax.rem(col + d, col_count) for d in range(1, col_count)]

    def wait_passes(g):
        wait_pass(g, 0)
        wait_pass(g, 1)

    for part in range(len(parts)):
        form(part)
    last = turns * HALVES - 1
    pending = []

    def settle():
        g = pending.pop(0)
        wait_passes(g)
        for c in others:
            transform(g, c)
        if g + HALVES > last:
            put_out(g % HALVES)

    for g in range(last + 1):
        for group in range(FARS // 2):
            forward(g, group)
        if len(pending) > 1:
            settle()
        for group in range(FARS // 2, FARS):
            forward(g, group)
        wait_near(g)
        transform(g, col)
        pending.append(g)
    put_out(last % HALVES)
    while len(pending) > 1:
        settle()
    wait_passes(last)
    for copy in tails:
        copy.wait()
    if fused:
        for h in range(HALVES):
            drain(acc_ref.at[h], out_sem.at[h])

    for i in range(2):
        drain(planes[i].at[pl.ds(0, row_count - 1)], wave_send.at[i])
    for copy in sent:
        copy.wait_send()
    drain(x_ref.at[:, 0, pl.ds(0, row_count - 1)], give_send.at[0])
    for d in range(1, col_count):
        drain(x_ref.at[:, 0], pass_send.at[0])

    @pl.when(col == 0)
    def _():
        for i in range(2):
            for c in range(1, col_count):
                over_col(i, c).wait_send()

    if not fused:
        for copy in own[2 * turns :]:
            copy.wait()


def whole(row_count, col_count, occ, vir, decays, window, factor):
    inner = group_size(row_count)
    outer = row_count // inner
    points = occ.shape[1] // row_count
    fused = points == NB * NC and row_count * col_count == NA and (row_count // 2) % (LANES // NB) == 0
    fused = fused and row_count % 2 == 0
    turns = 2 if fused else 1
    span = points // turns
    parts = tuple((turn, 0, span) for turn in range(turns))
    bands = (occ.shape[0], vir.shape[0])
    block_rows = row_count * HALF_ROWS
    bf16, f32 = jnp.bfloat16, jnp.float32
    dma = pltpu.SemaphoreType.DMA
    vmem = pl.BlockSpec(memory_space=pltpu.VMEM)
    hbm = pl.BlockSpec(memory_space=pltpu.HBM)
    x_shape = (turns * HALVES, col_count, row_count, HALF_ROWS, span)
    operands = [occ, vir, decays]
    in_specs = [hbm, hbm, vmem]
    scratch = [pltpu.VMEM((row_count, b, points), bf16) for b in bands]
    scratch += [pltpu.VMEM((outer, inner, b, window), bf16) for b in bands]
    scratch += [pltpu.VMEM((window, row_count * b), bf16) for b in bands]
    scratch += [
        pltpu.VMEM((HALVES, block_rows, span), f32),
        pltpu.VMEM((turns * HALVES, row_count, HALF_ROWS, span), bf16),
        pltpu.VMEM((span, span), bf16),
    ]
    if fused:
        line, angles = line_tables(col_count), angle_tables()
        depth = row_count * (span // NC)
        operands += [line, angles]
        in_specs += [hbm] * 2
        scratch += [
            pltpu.VMEM(x_shape, bf16),
            pltpu.VMEM(line.shape[1:], bf16),
            pltpu.VMEM(angles.shape, f32),
            pltpu.VMEM((2 * NAB, NAB), bf16),
            pltpu.VMEM((NC * R_BLOCK, row_count * (span // NC)), bf16),
        ]
        scratch += [pltpu.VMEM((HALVES, line.shape[1], NAB), f32)]
        scratch += [dma((2,)), dma((HALVES,)), dma((2 * col_count,))]
        out_shape = [jax.ShapeDtypeStruct((HALVES * line.shape[1] // 2 // PIECES, NAB), f32)] * (2 * PIECES)
        late = col_count - 1
        tails = [(late, row_count, HALF_ROWS, span)] + [(late, depth, NAB)] * 2 + [line.shape[1:]]
        out_shape += [jax.ShapeDtypeStruct(shape, bf16) for shape in tails]
    else:
        out_shape = [jax.ShapeDtypeStruct(x_shape, bf16)]
    places = max(1, col_count - 1)
    steps = outer - 1 + inner - 1
    scratch += [dma((2,)), dma((2, len(parts))), dma((2, places)), dma((2,))]
    scratch += [dma((2, steps))] * 2 + [dma((2, places))] * 2
    gives = turns * HALVES
    scratch += [dma((1,)), dma((gives, 1 + FARS)), dma((1,)), dma((gives, places, 2))]
    scratch += [dma((turns, 2)), dma((2,)), dma((gives,))]
    cfg = (row_count, col_count, inner, turns, parts, factor, fused)
    result = pl.pallas_call(
        functools.partial(whole_kernel, cfg),
        out_shape=out_shape,
        in_specs=in_specs,
        out_specs=[pl.BlockSpec(memory_space=pl.ANY) if fused else vmem] * len(out_shape),
        scratch_shapes=scratch,
        compiler_params=pltpu.CompilerParams(
            collective_id=0, has_side_effects=True, vmem_limit_bytes=VMEM_LIMIT
        ),
    )(*operands)
    return fused, result


def last_kernel(*refs):
    parts = refs[: 2 * PIECES]
    tail_x, tail_cos, tail_sin, tail_line = refs[2 * PIECES : 2 * PIECES + 4]
    re_out, im_out, lines_buf, *acc, sems = refs[2 * PIECES + 4 :]
    outs = (re_out, im_out)
    half = PIECES // HALVES
    rows = parts[0].shape[0]
    copies = []

    def put(i, p, src):
        copy = pltpu.make_async_copy(src, outs[i].at[pl.ds(p * rows, rows)], sems.at[i, p])
        copy.start()
        copies.append(copy)

    for i in range(2):
        for p in range(half):
            put(i, p, parts[i * PIECES + p])
    late = []
    for d in range(tail_x.shape[0]):
        blocks = [tail_x.at[d, a] for a in range(tail_x.shape[1])]
        late.append((spread(blocks, lines_buf, tail_line), tail_cos[d], tail_sin[d]))
    for n in range(half):
        p = half + n
        for i in range(2):
            total = parts[i * PIECES + p][...]
            for both, cosine, sine in late:
                some = both[(i * half + n) * rows : (i * half + n + 1) * rows]
                middle = some.shape[1] // 2
                total = total + dot(some[:, :middle], cosine) + dot(some[:, middle:], sine)
            acc[i][pl.ds(n * rows, rows), :] = total
            put(i, p, acc[i].at[pl.ds(n * rows, rows)])
    for copy in copies:
        copy.wait()


def last(operands):
    rows, lanes = operands[0].shape
    vmem = pl.BlockSpec(memory_space=pltpu.VMEM)
    tail_x = operands[2 * PIECES]
    acc = pltpu.VMEM((rows * PIECES // HALVES, lanes), jnp.float32)
    return pl.pallas_call(
        last_kernel,
        out_shape=[jax.ShapeDtypeStruct((rows * PIECES, lanes), jnp.float32)] * 2,
        in_specs=[vmem] * len(operands),
        out_specs=[pl.BlockSpec(memory_space=pltpu.HBM)] * 2,
        scratch_shapes=[
            pltpu.VMEM((NC * R_BLOCK, operands[2 * PIECES + 1].shape[1]), jnp.bfloat16),
            acc,
            acc,
            pltpu.SemaphoreType.DMA((2, PIECES)),
        ],
        compiler_params=pltpu.CompilerParams(vmem_limit_bytes=8 * 1024 * 1024),
    )(*operands)


def on_device(rows_dev, occupied_waves, virtual_waves, occupied_decay, virtual_decay):
    row_count = lax.axis_size("row")
    col_count = lax.axis_size("col")
    nocc, nvir = occupied_decay.shape[0], virtual_decay.shape[0]
    window = rows_dev * row_count
    points = occupied_waves.shape[1] // row_count
    factor = -1.0 / math.sqrt(nocc * nvir) / math.sqrt(NGRID)
    fused, result = whole(
        row_count,
        col_count,
        occupied_waves,
        virtual_waves,
        jnp.concatenate([occupied_decay, virtual_decay]).reshape(1, nocc + nvir),
        window,
        factor,
    )
    if fused:
        real_part, imag_part = last(result)
    else:
        x = result[0].reshape(HALVES, col_count * row_count, R_BLOCK, NC, points // NC)
        x = jnp.transpose(x, (3, 0, 2, 1, 4)).reshape(NC, rows_dev, NAB)
        real_part, imag_part = spectrum(x, line_tables(col_count))
    shape = (rows_dev, NC // col_count, NAB)
    return real_part.reshape(shape), imag_part.reshape(shape)


ROWS_DEV = 32


def solution(mesh):
    in_specs = (P("row", "col"), P("row", "col"), P(), P())
    out_specs = (P("row", "col", None), P("row", "col", None))
    return jax.shard_map(
        functools.partial(on_device, ROWS_DEV),
        mesh=mesh,
        in_specs=in_specs,
        out_specs=out_specs,
        check_vma=False,
    )
```
